512 devices in a mesh: seq: 64 (over z, x, core), tp: 8 (over y).
Axes of the slice: x: 4, y: 8, z: 8, core: 2. Of those that a mesh axis runs over, the one named last changes fastest.
Arguments:
- hidden_in: bfloat16 [8192, 4096], P('seq', 'tp'), may hold values from -64 to 64
- span_order: int32 [64], replicated, may hold values from 0 to 63, each once
- norm_gain: bfloat16 [4096], P('tp'), may hold values from 0.099609375 to 1.8984375
- w_query: bfloat16 [4096, 4096], P('seq', 'tp'), may hold values from -0.09375 to 0.09375
- bias_query: bfloat16 [4096], P('tp'), may hold values from -14 to 14
- key_value_weight: bfloat16 [4096, 2, 1024], P('seq', None, 'tp'), may hold values from -0.09375 to 0.09375
- bias_kv: bfloat16 [2, 1024], P(None, 'tp'), may hold values from -14 to 14
- w_out: bfloat16 [4096, 4096], P('tp', 'seq'), may hold values from -0.09375 to 0.09375
- post_gain: bfloat16 [4096], P('tp'), may hold values from 0.099609375 to 1.8984375
Outputs:
- attn_out: bfloat16 [8192, 4096], P('seq', 'tp')
- normed: bfloat16 [8192, 4096], P('seq', 'tp')
The draws below stay inside these ranges and needn't reach their ends.
Inputs may be any that keep to these rules, and one draw needn't show every extreme that they name: Each span number appears once; row r of hidden_in belongs to span span_order[r // 128].
All inputs are finite; a program needn't handle non-finite values.
Results may differ from the reference program's by a relative error of at most 0.014.
Values may be sent and summed in bfloat16 or wider, within the bound.
A program may use at most 64 MiB of HBM per device.

```python
import math
import jax
import jax.numpy as jnp
from jax import lax

MODEL_WIDTH = 4096
QUERY_HEADS = 32
KEY_VALUE_HEADS = 8
HEAD_SIZE = 128
GROUP = 4
TOK_DEV = 128
SEQ = 8192
N_SEQ = 64
N_TP = 8


def draw_hidden_in(key, part):
    base_key, column_key, row_key = jax.random.split(key, 3)
    column_ids = jnp.arange(MODEL_WIDTH, dtype=jnp.float32) / MODEL_WIDTH
    base = jnp.clip(jax.random.normal(base_key, (SEQ, MODEL_WIDTH), jnp.float32), -4.0, 4.0)
    ramp = jnp.exp(0.5 * math.log(3.0) * column_ids)
    ramp = ramp / jnp.mean(ramp)
    columns = jnp.exp(jax.random.uniform(column_key, (MODEL_WIDTH,), jnp.float32, -1.1513, 1.1513))
    rows = jnp.exp(jax.random.uniform(row_key, (SEQ, 1), jnp.float32, -1.1513, 1.1513))
    field = jnp.clip(base * rows * (columns * ramp)[None, :], -64.0, 64.0)
    return field.astype(jnp.bfloat16)


def draw_bias_query(key, part):
    random_jitter = jax.random.normal(jax.random.fold_in(key, 11), (QUERY_HEADS * HEAD_SIZE,), jnp.float32)
    return jnp.clip(0.5 * random_jitter, -2.0, 2.0).astype(jnp.bfloat16)


def draw_bias_kv(key, part):
    random_jitter = jax.random.normal(jax.random.fold_in(key, 13), (2, KEY_VALUE_HEADS * HEAD_SIZE), jnp.float32)
    return jnp.clip(0.5 * random_jitter, -2.0, 2.0).astype(jnp.bfloat16)


def steps_of(stream_key, extent, pieces, low, top_value):
    factor_of = 1.0
    for position, shards_of in pieces:
        heights = jax.random.uniform(jax.random.fold_in(jax.random.fold_in(stream_key, 6), position), (shards_of,), jnp.float32, low / len(pieces), top_value / len(pieces))
        factor_of = factor_of * jnp.repeat(jnp.exp(heights), extent[position] // shards_of).reshape((-1,) + (1,) * (len(extent) - 1 - position))
    return factor_of


def noise(rng, dims, deviation, most, cuts=(), held_as=jnp.bfloat16):
    factor_of = steps_of(rng, dims, cuts, -0.22, 0.18) if cuts else 1.0
    result = jax.random.normal(rng, dims, jnp.float32) * deviation * factor_of
    return jnp.minimum(jnp.maximum(result, -most), most).astype(held_as)


def setup_inputs(seed: int = 0) -> dict:
    arg_keys = jax.random.split(jax.random.key(seed), 10)
    hidden_in = draw_hidden_in(jax.random.fold_in(arg_keys[9], 71), 0)
    span_order = jax.random.permutation(arg_keys[1], N_SEQ).astype(jnp.int32)
    norm_gain = jnp.clip(1.0 + 0.18 * jax.random.normal(arg_keys[2], (MODEL_WIDTH,), jnp.float32), 0.099609375, 1.8984375).astype(jnp.bfloat16)
    w_query = noise(arg_keys[3], (MODEL_WIDTH, QUERY_HEADS * HEAD_SIZE), MODEL_WIDTH ** -0.5, 0.09375, ((0, 64), (1, 8)))
    bias_query = draw_bias_query(jax.random.fold_in(arg_keys[9], 71), 0)
    key_value_weight = noise(arg_keys[5], (MODEL_WIDTH, 2, KEY_VALUE_HEADS * HEAD_SIZE), MODEL_WIDTH ** -0.5, 0.09375, ((0, 64), (2, 8)))
    bias_kv = draw_bias_kv(jax.random.fold_in(arg_keys[9], 71), 0)
    w_out = noise(arg_keys[7], (QUERY_HEADS * HEAD_SIZE, MODEL_WIDTH), (QUERY_HEADS * HEAD_SIZE) ** -0.5, 0.09375, ((0, 8), (1, 64)))
    post_gain = jnp.clip(1.0 + 0.18 * jax.random.normal(arg_keys[8], (MODEL_WIDTH,), jnp.float32), 0.099609375, 1.8984375).astype(jnp.bfloat16)
    return dict(hidden_in=hidden_in, span_order=span_order, norm_gain=norm_gain, w_query=w_query, bias_query=bias_query, key_value_weight=key_value_weight, bias_kv=bias_kv, w_out=w_out, post_gain=post_gain)


eps = 1e-06
rope_base = 1000000.0

def apply_rotary(field, token_positions):
    half = field.shape[-1] // 2
    inverse = jnp.exp(-math.log(rope_base) * jnp.arange(half, dtype=jnp.float32) / half)
    angles = token_positions.astype(jnp.float32)[:, None] * inverse[None, :]
    cosine = jnp.cos(angles)[:, None, :]
    sine = jnp.sin(angles)[:, None, :]
    first = field[..., :half]
    second = field[..., half:]
    return jnp.concatenate([first * cosine - second * sine, second * cosine + first * sine], axis=-1)

def reference(hidden_in, span_order, norm_gain, w_query, bias_query, key_value_weight, bias_kv, w_out, post_gain):
    sequence_length = hidden_in.shape[0]
    row_ids = jnp.arange(sequence_length, dtype=jnp.int32)
    token_positions = (span_order[row_ids // TOK_DEV] * TOK_DEV + row_ids % TOK_DEV).astype(jnp.int32)
    local = hidden_in.astype(jnp.float32)
    meansq = lax.optimization_barrier(jnp.mean(local * local, axis=1, keepdims=True))
    normed_in = (local * lax.rsqrt(meansq + eps) * norm_gain.astype(jnp.float32)[None, :]).astype(jnp.bfloat16)
    query_proj = jnp.dot(normed_in, w_query, preferred_element_type=jnp.float32) + bias_query.astype(jnp.float32)[None, :]
    queries = apply_rotary(query_proj.reshape(sequence_length, QUERY_HEADS, HEAD_SIZE), token_positions).astype(jnp.bfloat16)
    key_projected = jnp.dot(normed_in, key_value_weight[:, 0, :], preferred_element_type=jnp.float32) + bias_kv[0].astype(jnp.float32)[None, :]
    value_projected = jnp.dot(normed_in, key_value_weight[:, 1, :], preferred_element_type=jnp.float32) + bias_kv[1].astype(jnp.float32)[None, :]
    rotated_keys = apply_rotary(key_projected.reshape(sequence_length, KEY_VALUE_HEADS, HEAD_SIZE), token_positions).astype(jnp.bfloat16)
    value_rows = value_projected.astype(jnp.bfloat16).reshape(sequence_length, KEY_VALUE_HEADS, HEAD_SIZE)
    query_major = queries.transpose(1, 0, 2)
    key_major = jnp.repeat(rotated_keys.transpose(1, 0, 2), GROUP, axis=0)
    value_major = jnp.repeat(value_rows.transpose(1, 0, 2), GROUP, axis=0)
    allowed = token_positions[None, :] <= token_positions[:, None]
    scale = 1.0 / math.sqrt(HEAD_SIZE)

    def one_head(triple):
        query_one, key_one, value_one = triple
        scores = jnp.dot(query_one, key_one.T, preferred_element_type=jnp.float32) * scale
        scores = jnp.where(allowed, scores, -jnp.inf)
        peak = lax.optimization_barrier(jnp.max(scores, axis=1, keepdims=True))
        weights = jnp.where(allowed, jnp.exp(scores - peak), 0.0)
        totals = lax.optimization_barrier(jnp.sum(weights, axis=1, keepdims=True))
        summed = jnp.dot(weights.astype(jnp.bfloat16), value_one, preferred_element_type=jnp.float32)
        return (summed / totals).astype(jnp.bfloat16)
    attended = lax.map(one_head, (query_major, key_major, value_major))
    attended = attended.transpose(1, 0, 2).reshape(sequence_length, QUERY_HEADS * HEAD_SIZE)
    part_rows = QUERY_HEADS * HEAD_SIZE // N_TP
    mixed = jnp.zeros((sequence_length, MODEL_WIDTH), jnp.float32)
    for group in range(N_TP):
        lower = group * part_rows
        piece = jnp.dot(attended[:, lower:lower + part_rows], w_out[lower:lower + part_rows, :], preferred_element_type=jnp.float32)
        mixed = mixed + lax.optimization_barrier(piece.astype(jnp.bfloat16)).astype(jnp.float32)
    attn_out = mixed.astype(jnp.bfloat16)
    stream = local + mixed
    post_sq = lax.optimization_barrier(jnp.mean(stream * stream, axis=1, keepdims=True))
    normed = (stream * lax.rsqrt(post_sq + eps) * post_gain.astype(jnp.float32)[None, :]).astype(jnp.bfloat16)
    return (attn_out, normed)
```

```python
import functools
import math

import jax
import jax.numpy as jnp
from jax import lax
from jax.experimental import pallas as pl
from jax.experimental.pallas import tpu as pltpu
from jax.sharding import Mesh
from jax.sharding import PartitionSpec as P

MODEL_WIDTH = 4096
HEAD_SIZE = 128
GROUP = 4
TOK = 128
NZ, NX, NC, NY = 8, 4, 2, 8
PLANE = NZ * NX
BLOCKS = PLANE * NC
COLS = MODEL_WIDTH // NY
WROWS = MODEL_WIDTH // BLOCKS
SUBS = 2
SEQ = ("z", "x", "c")
MESH_ID = pl.DeviceIdType.MESH

eps = 1e-06
rope_base = 1000000.0
exponent_scale = math.log2(math.e) / math.sqrt(HEAD_SIZE)


def x_first_tree():
    parent = {(1, 0): (0, 0), (-1, 0): (0, 0), (2, 0): (1, 0)}
    for dx in (0, 1, -1, 2):
        for dz in (1, 2, 3):
            parent[dx, dz] = (dx, dz - 1)
            parent[dx, -dz] = (dx, 1 - dz)
        parent[dx, 4] = (dx, 3) if dx in (0, 1) else (dx, -3)
    return parent


def z_first_tree():
    parent = {(0, 4): (0, 3)}
    for dz in (1, 2, 3):
        parent[0, dz] = (0, dz - 1)
        parent[0, -dz] = (0, 1 - dz)
    for dz in range(-3, 5):
        parent[1, dz] = (0, dz)
        parent[-1, dz] = (0, dz)
        parent[2, dz] = (1, dz) if dz % 2 == 0 else (-1, dz)
    return parent


def levels_of(parent):
    depth = {(0, 0): 0}

    def depth_of(o):
        if o not in depth:
            depth[o] = depth_of(parent[o]) + 1
        return depth[o]

    levels = [[] for _ in range(7)]
    for o in [(0, 0)] + list(parent):
        levels[depth_of(o)].append(o)
    return levels


def slot(o):
    return (o[1] % NZ) * NX + o[0] % NX


class Gather:
    def __init__(self, parent, buf, arrive, handed, sent, place, by_row):
        self.parent, self.buf, self.arrive = parent, buf, arrive
        self.handed, self.sent, self.place, self.by_row = handed, sent, place, by_row
        self.levels = levels_of(parent)

    def index(self, o):
        z, x, c, y = self.place
        return (lax.rem(z - o[1] + NZ, NZ) * NX + lax.rem(x - o[0] + NX, NX)) * NC + c

    def to(self, src, device, sem):
        return pltpu.make_async_remote_copy(
            src_ref=src,
            dst_ref=src,
            send_sem=self.sent.at[0],
            recv_sem=sem,
            device_id=device,
            device_id_type=MESH_ID,
        )

    def send(self, o):
        z, x, c, y = self.place
        block = self.buf.at[self.index(o)]
        for child, above in self.parent.items():
            if above == o:
                dx = (child[0] - o[0] + 1) % NX - 1
                dz = (child[1] - o[1] + 1) % NZ - 1
                near = (lax.rem(z + dz + NZ, NZ), lax.rem(x + dx + NX, NX), c, y)
                self.to(block, near, self.arrive.at[slot(child)]).start()
        row = o[1] % NZ if self.by_row else 0
        self.to(block, (z, x, 1 - c, y), self.handed.at[row]).start()

    def round(self, level):
        z, x, c, y = self.place
        for o in self.levels[level]:
            if level:
                block = self.buf.at[self.index(o)]
                self.to(block, (z, x, 1 - c, y), self.arrive.at[slot(o)]).wait_recv()
            self.send(o)

    def wait_handed(self, row=0):
        part = self.buf.at[pl.ds(0, NX if self.by_row else PLANE)]
        pltpu.make_async_copy(part, part, self.handed.at[row]).wait()

    def wait_sent(self):
        part = self.buf.at[pl.ds(0, BLOCKS - 1)]
        pltpu.make_async_copy(part, part, self.sent.at[0]).wait()


def kernel(
    hidden_ref,
    gain_ref,
    wq_ref,
    wkv_ref,
    wo_ref,
    bq_ref,
    bkv_ref,
    post_ref,
    rope_ref,
    qpos_ref,
    kpos_ref,
    attn_ref,
    normed_ref,
    hid,
    gains,
    wkv,
    wq,
    kv,
    wo,
    u,
    inv,
    qs,
    top,
    total,
    acc,
    attended,
    plus_in,
    minus_in,
    plus_out,
    minus_out,
    stats,
    local_sem,
    hid_arrive,
    hid_sent,
    gain_arrive,
    gain_sent,
    wkv_arrive,
    wkv_handed,
    wkv_sent,
    wq_arrive,
    wq_handed,
    wq_sent,
    kv_arrive,
    kv_handed,
    kv_sent,
    wo_arrive,
    wo_handed,
    wo_sent,
    plus_arrive,
    plus_sent,
    minus_arrive,
    minus_sent,
    stats_arrive,
    stats_sent,
):
    z, x, c, y = (lax.axis_index(n) for n in ("z", "x", "c", "y"))
    place = (z, x, c, y)
    me = (z * NX + x) * NC + c

    def y_near(d):
        return (z, x, c, lax.rem(y + d + NY, NY))

    def y_at(d):
        return lax.rem(y + d + NY, NY)

    starts = [
        pltpu.make_async_copy(wkv_ref, wkv.at[me], local_sem.at[0]),
        pltpu.make_async_copy(hidden_ref, hid.at[y], local_sem.at[1]),
        pltpu.make_async_copy(wq_ref, wq.at[me], local_sem.at[2]),
    ]
    for s in starts:
        s.start()
    gains[y] = jnp.broadcast_to(gain_ref[...].astype(jnp.float32), (8, COLS))
    barrier = pltpu.get_barrier_semaphore()
    friends = [(z, x, 1 - c, y)]
    friends += [(lax.rem(z + d, NZ), x, c, y) for d in (1, NZ - 1)]
    friends += [(z, lax.rem(x + d, NX), c, y) for d in (1, NX - 1)]
    friends += [(z, x, c, lax.rem(y + d, NY)) for d in range(1, NY)]
    for f in friends:
        pl.semaphore_signal(barrier, inc=1, device_id=f, device_id_type=MESH_ID)
    pl.semaphore_wait(barrier, len(friends))

    tree_a, tree_b = x_first_tree(), z_first_tree()
    g_wkv = Gather(tree_a, wkv, wkv_arrive, wkv_handed, wkv_sent, place, False)
    g_wq = Gather(tree_b, wq, wq_arrive, wq_handed, wq_sent, place, False)
    g_kv = Gather(tree_a, kv, kv_arrive, kv_handed, kv_sent, place, True)
    g_wo = Gather(tree_b, wo, wo_arrive, wo_handed, wo_sent, place, False)

    def remote(src, dst, sent, arrive, device):
        return pltpu.make_async_remote_copy(
            src_ref=src,
            dst_ref=dst,
            send_sem=sent,
            recv_sem=arrive,
            device_id=device,
            device_id_type=MESH_ID,
        )

    def hid_copy(step, sign):
        block = hid.at[y_at(-sign * step)]
        if step == 3:
            block = block.at[pl.ds(0 if sign > 0 else TOK // 2, TOK // 2)]
        k = step * 2 + (sign > 0)
        return remote(block, block, hid_sent.at[k], hid_arrive.at[k], y_near(sign))

    def hid_send(step):
        for sign in (1, -1):
            hid_copy(step, sign).start()

    def hid_wait(step):
        for sign in (1, -1):
            block = hid.at[y_at(-sign * (step + 1))]
            if step == 3:
                block = block.at[pl.ds(0 if sign > 0 else TOK // 2, TOK // 2)]
            k = step * 2 + (sign > 0)
            remote(block, block, hid_sent.at[k], hid_arrive.at[k], y_near(sign)).wait_recv()

    def gain_copy(d, source):
        block = gains.at[source]
        return remote(block, block, gain_sent.at[d], gain_arrive.at[d], y_near(d))

    starts[0].wait()
    g_wkv.round(0)
    starts[1].wait()
    hid_send(0)
    for d in range(1, NY):
        gain_copy(d, y).start()
    starts[2].wait()
    g_wq.round(0)

    wo[me] = wo_ref[...].astype(jnp.float32).T.astype(jnp.bfloat16)

    def prepare(source, d, first=False):
        if d:
            gain_copy(d % NY, source).wait_recv()
        h = hid[source].astype(jnp.float32)
        g = gains[source][0:1, :]
        u[source] = (h * g).astype(jnp.bfloat16)
        squares = h * h
        part = squares[:, 0:128]
        for k in range(1, COLS // 128):
            part = part + squares[:, k * 128 : (k + 1) * 128]
        inv[...] = part if first else inv[...] + part

    prepare(y, 0, True)
    for r in range(1, 5):
        g_wkv.round(r)
        hid_wait(r - 1)
        if r < 4:
            hid_send(r)
            prepare(y_at(r), -r)
            prepare(y_at(-r), r)
        else:
            prepare(y_at(4), 4)
        g_wq.round(r)
    g_wkv.round(5)
    g_wq.round(5)
    g_wkv.round(6)
    g_wkv.wait_handed()

    row_sum = jnp.sum(inv[...], axis=1, keepdims=True)
    row_scale = lax.rsqrt(row_sum / MODEL_WIDTH + eps)
    inv[...] = jnp.broadcast_to(row_scale, (TOK, 128))

    def project(weights, width):
        def step(k, total):
            block = weights[pl.ds(k * (BLOCKS // NY), BLOCKS // NY)].reshape(COLS, width)
            return total + jnp.dot(u[k], block, preferred_element_type=jnp.float32)

        return lax.fori_loop(0, NY, step, jnp.zeros((TOK, width), jnp.float32))

    def rotate(head):
        return head * rope_ref[0] + pltpu.roll(head, HEAD_SIZE // 2, 1) * rope_ref[1]

    pair = project(wkv, 2 * HEAD_SIZE)
    scale = inv[...]
    keys = pair[:, :HEAD_SIZE] * scale + bkv_ref[0:1, :].astype(jnp.float32)
    values = pair[:, HEAD_SIZE:] * scale + bkv_ref[1:2, :].astype(jnp.float32)
    kv[me, :, 0:HEAD_SIZE] = rotate(keys).astype(jnp.bfloat16)
    kv[me, :, HEAD_SIZE : 2 * HEAD_SIZE] = values.astype(jnp.bfloat16)
    g_wq.round(6)
    g_kv.round(0)
    g_wo.round(0)
    g_wq.wait_handed()

    query = project(wq, COLS)
    for g in range(GROUP):
        lanes = slice(g * HEAD_SIZE, (g + 1) * HEAD_SIZE)
        one = query[:, lanes] * inv[...] + bq_ref[0:1, lanes].astype(jnp.float32)
        qs[g] = rotate(one).astype(jnp.bfloat16)

    def attend(row, first):
        seq_row = lax.rem(z - row + NZ, NZ)
        chunk = NX * NC * TOK

        def head(g, carry):
            block = kv[pl.ds(seq_row * NX * NC, NX * NC)].reshape(chunk, 2 * HEAD_SIZE)
            scores = lax.dot_general(
                qs[g],
                block[:, :HEAD_SIZE],
                (((1,), (1,)), ((), ())),
                preferred_element_type=jnp.float32,
            )
            allowed = kpos_ref[pl.ds(seq_row, 1), :] <= qpos_ref[:, 0:1]
            scores = jnp.where(allowed, scores * exponent_scale, -1e30)
            peak = jnp.max(scores, axis=1, keepdims=True)
            if not first:
                old = top[g][:, 0:1]
                peak = jnp.maximum(old, peak)
            weights = jnp.exp2(scores - peak)
            count = jnp.sum(weights, axis=1, keepdims=True)
            summed = jnp.dot(
                weights.astype(jnp.bfloat16),
                block[:, HEAD_SIZE:],
                preferred_element_type=jnp.float32,
            )
            if not first:
                factor = jnp.exp2(old - peak)
                count = count + total[g][:, 0:1] * factor
                summed = summed + acc[g] * factor
            top[g] = jnp.broadcast_to(peak, (TOK, 128))
            total[g] = jnp.broadcast_to(count, (TOK, 128))
            acc[g] = summed
            return carry

        lax.fori_loop(0, GROUP, head, 0)

    for r in range(1, 7):
        g_kv.round(r)
        g_wo.round(r)
        if r >= 2:
            for row in sorted({r - 2, 2 - r} if r < 6 else {4}):
                g_kv.wait_handed(row % NZ)
                attend(row, r == 2)
    for g in range(GROUP):
        attended[:, g * HEAD_SIZE : (g + 1) * HEAD_SIZE] = (acc[g] / total[g]).astype(jnp.bfloat16)
    g_wo.wait_handed()

    def partial(target):
        block = wo[pl.ds(target * (BLOCKS // NY), BLOCKS // NY)].reshape(COLS, COLS)
        return lax.dot_general(
            attended[...], block, (((1,), (1,)), ((), ())), preferred_element_type=jnp.float32
        )

    sub = TOK // SUBS
    half = COLS // 2

    def sum_copy(step, sign, piece):
        outs, ins, sent, arrive = (
            (plus_out, plus_in, plus_sent, plus_arrive)
            if sign > 0
            else (minus_out, minus_in, minus_sent, minus_arrive)
        )
        rows = pl.ds(piece * sub, sub)
        lanes = pl.ds(0, COLS)
        if step == 0:
            lanes = pl.ds(0 if sign > 0 else half, half)
        k = step * SUBS + piece
        return remote(
            outs.at[step, rows, lanes],
            ins.at[step, rows, lanes],
            sent.at[k],
            arrive.at[k],
            y_near(sign),
        )

    far = partial(y_at(4)).astype(jnp.bfloat16)
    plus_out[0, :, 0:half] = far[:, :half]
    minus_out[0, :, half:COLS] = far[:, half:]
    for piece in range(SUBS):
        sum_copy(0, 1, piece).start()
        sum_copy(0, -1, piece).start()
    for step in range(1, 4):
        terms = {1: partial(y_at(4 - step)), -1: partial(y_at(step - 4))}
        for piece in range(SUBS):
            rows = slice(piece * sub, (piece + 1) * sub)
            for sign in (1, -1):
                outs, ins = (plus_out, plus_in) if sign > 0 else (minus_out, minus_in)
                sum_copy(step - 1, sign, piece).wait_recv()
                term = terms[sign][rows]
                if step == 1:
                    lanes = slice(0, half) if sign > 0 else slice(half, COLS)
                    other = slice(half, COLS) if sign > 0 else slice(0, half)
                    got = ins[0, rows, lanes].astype(jnp.float32)
                    outs[1, rows, lanes] = (term[:, lanes] + got).astype(jnp.bfloat16)
                    outs[1, rows, other] = term[:, other].astype(jnp.bfloat16)
                else:
                    got = ins[step - 1, rows].astype(jnp.float32)
                    outs[step, rows] = (term + got).astype(jnp.bfloat16)
                sum_copy(step, sign, piece).start()
    own = partial(y)
    for piece in range(SUBS):
        rows = slice(piece * sub, (piece + 1) * sub)
        for sign in (1, -1):
            sum_copy(3, sign, piece).wait_recv()
        mixed = (
            own[rows]
            + plus_in[3, rows].astype(jnp.float32)
            + minus_in[3, rows].astype(jnp.float32)
        )
        attn_ref[rows, :] = mixed.astype(jnp.bfloat16)
        stream = hid[y, rows].astype(jnp.float32) + mixed
        squares = stream * stream
        part = squares[:, 0:128]
        for k in range(1, COLS // 128):
            part = part + squares[:, k * 128 : (k + 1) * 128]
        inv[rows, :] = part
        for g in range(GROUP):
            acc[g, rows, :] = stream[:, g * 128 : (g + 1) * 128]

    column = jnp.sum(inv[...], axis=1, keepdims=True)
    stats[y] = jnp.broadcast_to(column, (TOK, 128)).T[0:8, :]

    def stats_copy(d, source):
        block = stats.at[source]
        return remote(block, block, stats_sent.at[d], stats_arrive.at[d], y_near(d))

    for d in range(1, NY):
        stats_copy(d, y).start()
    for g in (g_wkv, g_wq, g_kv, g_wo):
        g.wait_sent()
    for step in range(4):
        for sign in (1, -1):
            hid_copy(step, sign).wait_send()
            for piece in range(SUBS):
                sum_copy(step, sign, piece).wait_send()
    for d in range(1, NY):
        gain_copy(d, y).wait_send()
    for d in range(1, NY):
        stats_copy(d, y_at(-d)).wait_recv()
    summed = stats[0]
    for k in range(1, NY):
        summed = summed + stats[k]
    rows = jnp.broadcast_to(summed[0:1, :], (128, TOK)).T
    scale = lax.rsqrt(rows / MODEL_WIDTH + eps)
    for g in range(GROUP):
        lanes = slice(g * 128, (g + 1) * 128)
        gain = post_ref[0:1, lanes].astype(jnp.float32)
        normed_ref[:, lanes] = (acc[g] * scale * gain).astype(jnp.bfloat16)
    for d in range(1, NY):
        stats_copy(d, y).wait_send()


def per_device(
    hidden_in,
    span_order,
    norm_gain,
    w_query,
    bias_query,
    key_value_weight,
    bias_kv,
    w_out,
    post_gain,
):
    seq_index = lax.axis_index(SEQ)
    own_span = jnp.sum(jnp.where(jnp.arange(BLOCKS) == seq_index, span_order, 0))
    inside = jnp.arange(TOK, dtype=jnp.int32)
    positions = own_span * TOK + inside
    key_positions = (span_order[:, None] * TOK + inside[None, :]).reshape(NZ, NX * NC * TOK)
    lane = jnp.arange(HEAD_SIZE, dtype=jnp.int32)
    pair = (lane % (HEAD_SIZE // 2)).astype(jnp.float32)
    inverse = jnp.exp(-math.log(rope_base) * pair / (HEAD_SIZE // 2))
    angles = positions.astype(jnp.float32)[:, None] * inverse[None, :]
    sign = jnp.where(lane < HEAD_SIZE // 2, -1.0, 1.0)
    rope = jnp.stack([jnp.cos(angles), jnp.sin(angles) * sign[None, :]])
    query_positions = jnp.broadcast_to(positions[:, None], (TOK, 128))

    bf16, f32 = jnp.bfloat16, jnp.float32
    vmem = pl.BlockSpec(memory_space=pltpu.VMEM)
    anywhere = pl.BlockSpec(memory_space=pl.ANY)
    dma = pltpu.SemaphoreType.DMA
    out = jax.ShapeDtypeStruct((TOK, COLS), bf16)
    gathers = []
    for rows in (1, 1, NZ, 1):
        gathers += [dma((PLANE,)), dma((rows,)), dma((1,))]
    return pl.pallas_call(
        kernel,
        out_shape=(out, out),
        in_specs=[anywhere, vmem, anywhere, anywhere] + [vmem] * 7,
        out_specs=(vmem, vmem),
        scratch_shapes=[
            pltpu.VMEM((NY, TOK, COLS), bf16),
            pltpu.VMEM((NY, 8, COLS), f32),
            pltpu.VMEM((BLOCKS, WROWS, 2 * HEAD_SIZE), bf16),
            pltpu.VMEM((BLOCKS, WROWS, COLS), bf16),
            pltpu.VMEM((BLOCKS, TOK, 2 * HEAD_SIZE), bf16),
            pltpu.VMEM((BLOCKS, WROWS, COLS), bf16),
            pltpu.VMEM((NY, TOK, COLS), bf16),
            pltpu.VMEM((TOK, 128), f32),
            pltpu.VMEM((GROUP, TOK, HEAD_SIZE), bf16),
            pltpu.VMEM((GROUP, TOK, 128), f32),
            pltpu.VMEM((GROUP, TOK, 128), f32),
            pltpu.VMEM((GROUP, TOK, 128), f32),
            pltpu.VMEM((TOK, COLS), bf16),
            pltpu.VMEM((4, TOK, COLS), bf16),
            pltpu.VMEM((4, TOK, COLS), bf16),
            pltpu.VMEM((4, TOK, COLS), bf16),
            pltpu.VMEM((4, TOK, COLS), bf16),
            pltpu.VMEM((NY, 8, 128), f32),
            dma((3,)),
            dma((8,)),
            dma((8,)),
            dma((NY,)),
            dma((NY,)),
            *gathers,
            dma((4 * SUBS,)),
            dma((4 * SUBS,)),
            dma((4 * SUBS,)),
            dma((4 * SUBS,)),
            dma((NY,)),
            dma((NY,)),
        ],
        compiler_params=pltpu.CompilerParams(
            collective_id=0, has_side_effects=True, vmem_limit_bytes=56 << 20
        ),
    )(
        hidden_in,
        norm_gain.reshape(1, COLS),
        w_query,
        key_value_weight.reshape(WROWS, 2 * HEAD_SIZE),
        w_out,
        bias_query.reshape(1, COLS),
        bias_kv,
        post_gain.reshape(1, COLS),
        rope,
        query_positions,
        key_positions,
    )


def solution(mesh):
    torus = Mesh(mesh.devices.reshape(NZ, NX, NC, NY), ("z", "x", "c", "y"))
    in_specs = (
        P(SEQ, "y"),
        P(),
        P("y"),
        P(SEQ, "y"),
        P("y"),
        P(SEQ, None, "y"),
        P(None, "y"),
        P("y", SEQ),
        P("y"),
    )
    out_specs = (P(SEQ, "y"), P(SEQ, "y"))
    return jax.shard_map(
        per_device, mesh=torus, in_specs=in_specs, out_specs=out_specs, check_vma=False
    )
```

```python
import heapq
import math

import jax
import jax.numpy as jnp
import numpy as np
from jax import lax
from jax.experimental import pallas as pl
from jax.experimental.pallas import tpu as pltpu
from jax.sharding import Mesh
from jax.sharding import PartitionSpec as P

MODEL_WIDTH = 4096
HEAD_SIZE = 128
GROUP = 4
TOK = 128
NZ, NX, NC, NY = 8, 4, 2, 8
PLANE = NZ * NX
BLOCKS = PLANE * NC
COLS = MODEL_WIDTH // NY
WROWS = MODEL_WIDTH // BLOCKS
SUBS = 4
HALVES = 2
SEQ = ("z", "x", "c")
MESH_ID = pl.DeviceIdType.MESH

eps = 1e-06
rope_base = 1000000.0
exponent_scale = math.log2(math.e) / math.sqrt(HEAD_SIZE)

RATE, HOP, FURTHER, HOP_Y, HAND = 46.6, 3.3, 0.7, 2.1, 1.6
WO_START = 12.0


def x_then_z(direct_x):
    parent = {(2, 0): (0, 0) if direct_x else (1, 0), (1, 0): (0, 0), (-1, 0): (0, 0)}
    for dx in (0, 1, -1, 2):
        for dz in (1, 2, 3):
            parent[dx, dz] = (dx, dz - 1)
            parent[dx, -dz] = (dx, 1 - dz)
        parent[dx, 4] = (dx, 3) if dx in (0, 1) else (dx, -3)
    return parent


def z_then_x(reach):
    parent = {}
    for far in (4, 3, -3, 2, -2, 1, -1):
        step = (abs(far) - 1) // reach * reach
        parent[0, far] = (0, step if far > 0 else -step)
    for dz in range(-3, 5):
        parent[1, dz] = (0, dz)
        parent[-1, dz] = (0, dz)
        parent[2, dz] = (1, dz) if dz % 2 == 0 else (-1, dz)
    return parent


TREES = {
    "wkv": z_then_x(4),
    "wq": x_then_z(True),
    "wo": z_then_x(1),
    "k": z_then_x(2),
    "v": x_then_z(False),
}
KB = {"wkv": 32, "wq": 64, "wo": 64, "k": 32, "v": 32}


def away(child, parent):
    dx = (child[0] - parent[0] + 1) % NX - 1
    dz = (child[1] - parent[1] + 3) % NZ - 3
    return dx, dz


def children_of(tree):
    below = {}
    for child, parent in tree.items():
        below.setdefault(parent, []).append(child)
    return below


def planned_steps():
    below = {g: children_of(t) for g, t in TREES.items()}
    free, heap, steps = {}, [], []
    got, tail = dict.fromkeys(TREES, 0), dict.fromkeys(TREES, 0.0)
    rows_in, waiting = {}, []
    now, hidden_left = 0.0, 6 * HALVES + 2
    keys_done = query_done = own_row_done = False

    def push(t, *what):
        heapq.heappush(heap, (round(t, 6), len(steps), len(heap), what))

    def transfer(route, kb, latency):
        end, hops = now, 0
        for link, n in route:
            free[link] = max(free.get(link, 0.0), now) + kb * n / RATE
            end, hops = max(end, free[link]), hops + n
        return end + latency + FURTHER * (hops - 1)

    push(0.0, "wkv", (0, 0))
    push(0.0, "wq", (0, 0))
    push(WO_START, "wo", (0, 0))
    for piece in range(HALVES):
        for sign in (1, -1):
            push(0.05, "hid", 0, sign, piece)
    while True:
        ahead = heap[0][0] if heap else math.inf
        keys_at = max(now, tail["wkv"] + HAND)
        query_at = max(now, tail["wq"] + HAND)
        if not keys_done and got["wkv"] == PLANE and not hidden_left and ahead >= keys_at - 0.3:
            now, keys_done = keys_at + 1.8, True
            steps.append(("keys",))
            push(now, "k", (0, 0))
            push(now + 0.01, "v", (0, 0))
            continue
        if keys_done and not query_done and got["wq"] == PLANE and ahead >= query_at - 0.3:
            now, query_done = query_at + 2.5, True
            steps.append(("query",))
            continue
        able = [w for w in waiting if own_row_done or w[1] == 0]
        if query_done and able and ahead >= max(now, able[0][0]) - 0.2:
            waiting.remove(able[0])
            now = max(now, able[0][0]) + 0.9
            own_row_done = True
            steps.append(("attend", able[0][1]))
            continue
        if not heap:
            return steps
        at, _, _, what = heapq.heappop(heap)
        now = max(now, at) + 0.03
        steps.append(what)
        if what[0] == "hid":
            _, hop, sign, piece = what
            if hop:
                hidden_left -= 1
                now += 0.25 / HALVES
            if hop < 3 or (hop == 3 and piece == (sign < 0)):
                route = [("y+" if sign > 0 else "y-", 1)]
                kb = TOK / HALVES
                push(transfer(route, kb, HOP_Y), "hid", hop + 1, sign, piece)
            continue
        g, o = what
        got[g] += 1
        tail[g] = max(tail[g], now)
        for child in below[g].get(o, ()):
            dx, dz = away(child, o)
            route = [("x+" if dx > 0 else "x-", abs(dx))] if dx else []
            route += [("z+" if dz > 0 else "z-", abs(dz))] if dz else []
            now += 0.03
            push(transfer(route, KB[g], HOP), g, child)
        now += 0.03
        if g in ("k", "v"):
            rows_in[o[1]] = rows_in.get(o[1], 0) + 1
            if rows_in[o[1]] == 2 * NX:
                waiting.append((now + HAND, o[1]))


class Gather:
    def __init__(self, tree, buf, arrive, handed, sent, place, by_row):
        self.below, self.buf, self.arrive = children_of(tree), buf, arrive
        self.handed, self.sent, self.place, self.by_row = handed, sent, place, by_row

    def index(self, o):
        z, x, c, y = self.place
        return (lax.rem(z - o[1] + NZ, NZ) * NX + lax.rem(x - o[0] + NX, NX)) * NC + c

    def slot(self, o):
        return (o[1] % NZ) * NX + o[0] % NX

    def to(self, src, device, sem):
        return pltpu.make_async_remote_copy(
            src_ref=src,
            dst_ref=src,
            send_sem=self.sent.at[0],
            recv_sem=sem,
            device_id=device,
            device_id_type=MESH_ID,
        )

    def arrived(self, o):
        z, x, c, y = self.place
        block = self.buf.at[self.index(o)]
        partner = (z, x, 1 - c, y)
        if o != (0, 0):
            self.to(block, partner, self.arrive.at[self.slot(o)]).wait_recv()
        for child in self.below.get(o, ()):
            dx, dz = away(child, o)
            near = (lax.rem(z + dz + NZ, NZ), lax.rem(x + dx + NX, NX), c, y)
            self.to(block, near, self.arrive.at[self.slot(child)]).start()
        row = o[1] % NZ if self.by_row else 0
        self.to(block, partner, self.handed.at[row]).start()

    def wait_handed(self, row=0):
        part = self.buf.at[pl.ds(0, NX if self.by_row else PLANE)]
        pltpu.make_async_copy(part, part, self.handed.at[row]).wait()

    def wait_sent(self):
        part = self.buf.at[pl.ds(0, BLOCKS - 1)]
        pltpu.make_async_copy(part, part, self.sent.at[0]).wait()


def kernel(
    hidden_ref,
    wq_ref,
    wkv_ref,
    wo_ref,
    span_ref,
    gain_ref,
    bq_ref,
    bkv_ref,
    inside_ref,
    spans_ref,
    mixed_ref,
    scale_ref,
    hid,
    gains,
    wkv,
    wq,
    wo,
    ks,
    vs,
    u,
    inv,
    rope,
    kpos,
    qs,
    top,
    total,
    acc,
    attended,
    plus_in,
    minus_in,
    plus_out,
    minus_out,
    stats,
    local_sem,
    hid_arrive,
    hid_sent,
    gain_arrive,
    gain_sent,
    wkv_arrive,
    wkv_handed,
    wkv_sent,
    wq_arrive,
    wq_handed,
    wq_sent,
    wo_arrive,
    wo_handed,
    wo_sent,
    k_arrive,
    k_handed,
    k_sent,
    v_arrive,
    v_handed,
    v_sent,
    plus_arrive,
    plus_sent,
    minus_arrive,
    minus_sent,
    stats_arrive,
    stats_sent,
):
    z, x, c, y = (lax.axis_index(n) for n in ("z", "x", "c", "y"))
    place = (z, x, c, y)
    me = (z * NX + x) * NC + c

    def y_near(d):
        return (z, x, c, lax.rem(y + d + NY, NY))

    def y_at(d):
        return lax.rem(y + d + NY, NY)

    barrier = pltpu.get_barrier_semaphore()
    friends = [(z, x, 1 - c, y)]
    friends += [(lax.rem(z + d, NZ), x, c, y) for d in range(1, NZ)]
    friends += [(z, lax.rem(x + d, NX), c, y) for d in range(1, NX)]
    friends += [(z, x, c, lax.rem(y + d, NY)) for d in range(1, NY)]
    for f in friends:
        pl.semaphore_signal(barrier, inc=1, device_id=f, device_id_type=MESH_ID)
    starts = {
        "wkv": pltpu.make_async_copy(wkv_ref, wkv.at[me], local_sem.at[0]),
        "hid": pltpu.make_async_copy(hidden_ref, hid.at[y], local_sem.at[1]),
        "wq": pltpu.make_async_copy(wq_ref, wq.at[me], local_sem.at[2]),
        "wo": pltpu.make_async_copy(wo_ref, wo.at[me], local_sem.at[3]),
    }
    for s in starts.values():
        s.start()

    own_gain = gain_ref[...].astype(jnp.float32).reshape(1, COLS)
    gains[y] = jnp.broadcast_to(own_gain, (8, COLS))
    own_span = span_ref[me]
    of_span = spans_ref[own_span]
    cos_s, sin_s = of_span[0:1, :], of_span[1:2, :]
    rope[0] = inside_ref[0] * cos_s - inside_ref[1] * sin_s
    lanes = lax.broadcasted_iota(jnp.int32, (TOK, 128), 1)
    sine = inside_ref[1] * cos_s + inside_ref[0] * sin_s
    rope[1] = jnp.where(lanes < HEAD_SIZE // 2, -sine, sine)
    token = lax.broadcasted_iota(jnp.int32, (1, TOK), 1)
    for row in range(NZ):
        for k in range(NX * NC):
            where = slice(k * TOK, (k + 1) * TOK)
            kpos[row : row + 1, where] = token + span_ref[row * NX * NC + k] * TOK
    inv[...] = jnp.zeros_like(inv)
    pl.semaphore_wait(barrier, len(friends))

    gathers = {
        "wkv": Gather(TREES["wkv"], wkv, wkv_arrive, wkv_handed, wkv_sent, place, False),
        "wq": Gather(TREES["wq"], wq, wq_arrive, wq_handed, wq_sent, place, False),
        "wo": Gather(TREES["wo"], wo, wo_arrive, wo_handed, wo_sent, place, False),
        "k": Gather(TREES["k"], ks, k_arrive, k_handed, k_sent, place, True),
        "v": Gather(TREES["v"], vs, v_arrive, v_handed, v_sent, place, True),
    }

    def remote(src, dst, sent, arrive, device):
        return pltpu.make_async_remote_copy(
            src_ref=src,
            dst_ref=dst,
            send_sem=sent,
            recv_sem=arrive,
            device_id=device,
            device_id_type=MESH_ID,
        )

    part_rows = TOK // HALVES

    def hid_copy(hop, sign, piece, arriving=False):
        source = y_at(-sign * (hop + 1 if arriving else hop))
        block = hid.at[source, pl.ds(piece * part_rows, part_rows)]
        k = (hop * HALVES + piece) * 2 + (sign > 0)
        return remote(block, block, hid_sent.at[k], hid_arrive.at[k], y_near(sign))

    def hid_goes(hop, sign, piece):
        return hop < 3 or (hop == 3 and piece == (sign < 0))

    def gain_copy(d, source):
        block = gains.at[source]
        return remote(block, block, gain_sent.at[d], gain_arrive.at[d], y_near(d))

    def prepare(source, piece):
        rows = slice(piece * part_rows, (piece + 1) * part_rows)
        h = hid[source, rows].astype(jnp.float32)
        u[source, rows] = (h * gains[source][0:1, :]).astype(jnp.bfloat16)
        squares = h * h
        part = squares[:, 0:128]
        for k in range(1, COLS // 128):
            part = part + squares[:, k * 128 : (k + 1) * 128]
        inv[rows] = inv[rows] + part

    def project(weights, width):
        def step(k, total):
            block = weights[pl.ds(k * (BLOCKS // NY), BLOCKS // NY)].reshape(COLS, width)
            return total + jnp.dot(u[k], block, preferred_element_type=jnp.float32)

        return lax.fori_loop(0, NY, step, jnp.zeros((TOK, width), jnp.float32))

    def rotate(head):
        return head * rope[0] + pltpu.roll(head, HEAD_SIZE // 2, 1) * rope[1]

    def make_keys():
        row_sum = jnp.sum(inv[...], axis=1, keepdims=True)
        inv[...] = jnp.broadcast_to(lax.rsqrt(row_sum / MODEL_WIDTH + eps), (TOK, 128))
        pair = project(wkv, 2 * HEAD_SIZE)
        scale = inv[...]
        keys = pair[:, :HEAD_SIZE] * scale + bkv_ref[0:1, :].astype(jnp.float32)
        values = pair[:, HEAD_SIZE:] * scale + bkv_ref[1:2, :].astype(jnp.float32)
        ks[me] = rotate(keys).astype(jnp.bfloat16)
        vs[me] = values.astype(jnp.bfloat16)

    def make_query():
        query = project(wq, COLS)
        bias = bq_ref[...].astype(jnp.float32).reshape(1, COLS)
        for g in range(GROUP):
            lanes = slice(g * HEAD_SIZE, (g + 1) * HEAD_SIZE)
            qs[g] = rotate(query[:, lanes] * inv[...] + bias[:, lanes]).astype(jnp.bfloat16)

    def attend(row):
        first = row == 0
        seq_row = lax.rem(z - row + NZ, NZ)
        chunk = NX * NC * TOK
        query_pos = lax.broadcasted_iota(jnp.int32, (TOK, 128), 0) + own_span * TOK

        def head(g, carry):
            scores = lax.dot_general(
                qs[g],
                ks[pl.ds(seq_row * NX * NC, NX * NC)].reshape(chunk, HEAD_SIZE),
                (((1,), (1,)), ((), ())),
                preferred_element_type=jnp.float32,
            )
            allowed = kpos[pl.ds(seq_row, 1), :] <= query_pos[:, 0:1]
            scores = jnp.where(allowed, scores * exponent_scale, -1e30)
            peak = jnp.max(scores, axis=1, keepdims=True)
            if not first:
                old = top[g][:, 0:1]
                peak = jnp.maximum(old, peak)
            weights = jnp.exp2(scores - peak)
            count = jnp.sum(weights, axis=1, keepdims=True)
            summed = jnp.dot(
                weights.astype(jnp.bfloat16),
                vs[pl.ds(seq_row * NX * NC, NX * NC)].reshape(chunk, HEAD_SIZE),
                preferred_element_type=jnp.float32,
            )
            if not first:
                factor = jnp.exp2(old - peak)
                count = count + total[g][:, 0:1] * factor
                summed = summed + acc[g] * factor
            top[g] = jnp.broadcast_to(peak, (TOK, 128))
            total[g] = jnp.broadcast_to(count, (TOK, 128))
            acc[g] = summed
            return carry

        lax.fori_loop(0, GROUP, head, 0)

    seen_gain = {0}
    for step in planned_steps():
        if step[0] == "hid":
            _, hop, sign, piece = step
            if hop == 0:
                if piece == 0 and sign > 0:
                    starts["hid"].wait()
                hid_copy(0, sign, piece).start()
                if piece == HALVES - 1 and sign < 0:
                    for d in range(1, NY):
                        gain_copy(d, y).start()
                    for k in range(HALVES):
                        prepare(y, k)
            else:
                hid_copy(hop - 1, sign, piece, True).wait_recv()
                if hid_goes(hop, sign, piece):
                    hid_copy(hop, sign, piece).start()
                d = sign * hop % NY
                if d not in seen_gain:
                    seen_gain.add(d)
                    gain_copy(d, y_at(-d)).wait_recv()
                prepare(y_at(-d), piece)
        elif step[0] == "keys":
            gathers["wkv"].wait_handed()
            make_keys()
        elif step[0] == "query":
            gathers["wq"].wait_handed()
            make_query()
        elif step[0] == "attend":
            gathers["k"].wait_handed(step[1] % NZ)
            gathers["v"].wait_handed(step[1] % NZ)
            attend(step[1])
        else:
            g, o = step
            if o == (0, 0) and g in starts:
                starts[g].wait()
            gathers[g].arrived(o)
    for g in range(GROUP):
        attended[:, g * HEAD_SIZE : (g + 1) * HEAD_SIZE] = (acc[g] / total[g]).astype(jnp.bfloat16)
    gathers["wo"].wait_handed()

    def partial(target):
        block = wo[pl.ds(target * (BLOCKS // NY), BLOCKS // NY)].reshape(COLS, COLS)
        return lax.dot_general(
            attended[...], block, (((1,), (1,)), ((), ())), preferred_element_type=jnp.float32
        )

    sub = TOK // SUBS
    half = COLS // 2

    def sum_copy(step, sign, piece):
        outs, ins, sent, arrive = (
            (plus_out, plus_in, plus_sent, plus_arrive)
            if sign > 0
            else (minus_out, minus_in, minus_sent, minus_arrive)
        )
        rows = pl.ds(piece * sub, sub)
        lanes = pl.ds(0, COLS)
        if step == 0:
            lanes = pl.ds(0 if sign > 0 else half, half)
        k = step * SUBS + piece
        return remote(
            outs.at[step, rows, lanes],
            ins.at[step, rows, lanes],
            sent.at[k],
            arrive.at[k],
            y_near(sign),
        )

    far = partial(y_at(4)).astype(jnp.bfloat16)
    plus_out[0, :, 0:half] = far[:, :half]
    minus_out[0, :, half:COLS] = far[:, half:]
    for piece in range(SUBS):
        sum_copy(0, 1, piece).start()
        sum_copy(0, -1, piece).start()
    for step in range(1, 4):
        terms = {1: partial(y_at(4 - step)), -1: partial(y_at(step - 4))}
        for piece in range(SUBS):
            rows = slice(piece * sub, (piece + 1) * sub)
            for sign in (1, -1):
                outs, ins = (plus_out, plus_in) if sign > 0 else (minus_out, minus_in)
                sum_copy(step - 1, sign, piece).wait_recv()
                term = terms[sign][rows]
                if step == 1:
                    lanes = slice(0, half) if sign > 0 else slice(half, COLS)
                    other = slice(half, COLS) if sign > 0 else slice(0, half)
                    got = ins[0, rows, lanes].astype(jnp.float32)
                    outs[1, rows, lanes] = (term[:, lanes] + got).astype(jnp.bfloat16)
                    outs[1, rows, other] = term[:, other].astype(jnp.bfloat16)
                else:
                    got = ins[step - 1, rows].astype(jnp.float32)
                    outs[step, rows] = (term + got).astype(jnp.bfloat16)
                sum_copy(step, sign, piece).start()
    own = partial(y)
    for piece in range(SUBS):
        rows = slice(piece * sub, (piece + 1) * sub)
        for sign in (1, -1):
            sum_copy(3, sign, piece).wait_recv()
        mixed = (
            own[rows]
            + plus_in[3, rows].astype(jnp.float32)
            + minus_in[3, rows].astype(jnp.float32)
        )
        mixed_ref[rows, :] = mixed
        stream = hid[y, rows].astype(jnp.float32) + mixed
        squares = stream * stream
        part = squares[:, 0:128]
        for k in range(1, COLS // 128):
            part = part + squares[:, k * 128 : (k + 1) * 128]
        inv[rows, :] = part

    column = jnp.sum(inv[...], axis=1, keepdims=True)
    stats[y] = jnp.broadcast_to(column, (TOK, 128)).T[0:8, :]

    def stats_copy(d, source):
        block = stats.at[source]
        return remote(block, block, stats_sent.at[d], stats_arrive.at[d], y_near(d))

    for d in range(1, NY):
        stats_copy(d, y).start()
    for g in gathers.values():
        g.wait_sent()
    for step in range(4):
        for sign in (1, -1):
            for piece in range(HALVES):
                if hid_goes(step, sign, piece):
                    hid_copy(step, sign, piece).wait_send()
            for piece in range(SUBS):
                sum_copy(step, sign, piece).wait_send()
    for d in range(1, NY):
        gain_copy(d, y).wait_send()
    for d in range(1, NY):
        stats_copy(d, y_at(-d)).wait_recv()
    summed = stats[0]
    for k in range(1, NY):
        summed = summed + stats[k]
    rows = jnp.broadcast_to(summed[0:1, :], (128, TOK)).T
    scale_ref[...] = lax.rsqrt(rows / MODEL_WIDTH + eps)
    for d in range(1, NY):
        stats_copy(d, y).wait_send()


def per_device(
    hidden_in,
    span_order,
    norm_gain,
    w_query,
    bias_query,
    key_value_weight,
    bias_kv,
    w_out,
    post_gain,
):
    half = HEAD_SIZE // 2
    inverse = rope_base ** (-(np.arange(HEAD_SIZE) % half) / half)
    row_angles = np.arange(TOK)[:, None] * inverse[None, :]
    span_angles = np.arange(BLOCKS)[:, None] * TOK * inverse[None, :]
    inside = np.stack([np.cos(row_angles), np.sin(row_angles)]).astype(np.float32)
    spans = np.stack([np.cos(span_angles), np.sin(span_angles)], axis=1).astype(np.float32)

    bf16, f32 = jnp.bfloat16, jnp.float32
    vmem = pl.BlockSpec(memory_space=pltpu.VMEM)
    smem = pl.BlockSpec(memory_space=pltpu.SMEM)
    anywhere = pl.BlockSpec(memory_space=pl.ANY)
    dma = pltpu.SemaphoreType.DMA
    gathers = []
    for rows in (1, 1, 1, NZ, NZ):
        gathers += [dma((PLANE,)), dma((rows,)), dma((1,))]
    mixed, scale = pl.pallas_call(
        kernel,
        out_shape=(
            jax.ShapeDtypeStruct((TOK, COLS), f32),
            jax.ShapeDtypeStruct((TOK, 128), f32),
        ),
        in_specs=[anywhere] * 4 + [smem] + [vmem] * 5,
        out_specs=(vmem, vmem),
        scratch_shapes=[
            pltpu.VMEM((NY, TOK, COLS), bf16),
            pltpu.VMEM((NY, 8, COLS), f32),
            pltpu.VMEM((BLOCKS, WROWS, 2 * HEAD_SIZE), bf16),
            pltpu.VMEM((BLOCKS, WROWS, COLS), bf16),
            pltpu.VMEM((BLOCKS, WROWS, COLS), bf16),
            pltpu.VMEM((BLOCKS, TOK, HEAD_SIZE), bf16),
            pltpu.VMEM((BLOCKS, TOK, HEAD_SIZE), bf16),
            pltpu.VMEM((NY, TOK, COLS), bf16),
            pltpu.VMEM((TOK, 128), f32),
            pltpu.VMEM((2, TOK, 128), f32),
            pltpu.VMEM((NZ, NX * NC * TOK), jnp.int32),
            pltpu.VMEM((GROUP, TOK, HEAD_SIZE), bf16),
            pltpu.VMEM((GROUP, TOK, 128), f32),
            pltpu.VMEM((GROUP, TOK, 128), f32),
            pltpu.VMEM((GROUP, TOK, 128), f32),
            pltpu.VMEM((TOK, COLS), bf16),
            pltpu.VMEM((4, TOK, COLS), bf16),
            pltpu.VMEM((4, TOK, COLS), bf16),
            pltpu.VMEM((4, TOK, COLS), bf16),
            pltpu.VMEM((4, TOK, COLS), bf16),
            pltpu.VMEM((NY, 8, 128), f32),
            dma((4,)),
            dma((8 * HALVES,)),
            dma((8 * HALVES,)),
            dma((NY,)),
            dma((NY,)),
            *gathers,
            dma((4 * SUBS,)),
            dma((4 * SUBS,)),
            dma((4 * SUBS,)),
            dma((4 * SUBS,)),
            dma((NY,)),
            dma((NY,)),
        ],
        compiler_params=pltpu.CompilerParams(
            collective_id=0, has_side_effects=True, vmem_limit_bytes=56 << 20
        ),
    )(
        hidden_in,
        w_query,
        key_value_weight.reshape(WROWS, 2 * HEAD_SIZE),
        w_out.T,
        span_order,
        norm_gain,
        bias_query,
        bias_kv,
        jnp.asarray(inside),
        jnp.asarray(spans),
    )
    stream = hidden_in.astype(f32) + mixed
    normed = stream * scale[:, 0:1] * post_gain.astype(f32)[None, :]
    return mixed.astype(bf16), normed.astype(bf16)


def solution(mesh):
    torus = Mesh(mesh.devices.reshape(NZ, NX, NC, NY), ("z", "x", "c", "y"))
    in_specs = (
        P(SEQ, "y"),
        P(),
        P("y"),
        P(SEQ, "y"),
        P("y"),
        P(SEQ, None, "y"),
        P(None, "y"),
        P("y", SEQ),
        P("y"),
    )
    out_specs = (P(SEQ, "y"), P(SEQ, "y"))
    return jax.shard_map(
        per_device, mesh=torus, in_specs=in_specs, out_specs=out_specs, check_vma=False
    )
```

```python
import heapq
import math

import jax
import jax.numpy as jnp
import numpy as np
from jax import lax
from jax.experimental import pallas as pl
from jax.experimental.pallas import tpu as pltpu
from jax.sharding import Mesh
from jax.sharding import PartitionSpec as P

MODEL_WIDTH = 4096
HEAD_SIZE = 128
GROUP = 4
TOK = 128
NZ, NX, NC, NY = 8, 4, 2, 8
PLANE = NZ * NX
BLOCKS = PLANE * NC
COLS = MODEL_WIDTH // NY
WROWS = MODEL_WIDTH // BLOCKS
SUBS = 4
HALVES = 2
SEQ = ("z", "x", "c")
MESH_ID = pl.DeviceIdType.MESH

eps = 1e-06
rope_base = 1000000.0
exponent_scale = math.log2(math.e) / math.sqrt(HEAD_SIZE)

RATE, HOP, FURTHER, HOP_Y, HAND = 46.6, 3.3, 0.7, 2.1, 1.6
WO_START = 12.0


def x_then_z(direct_x):
    parent = {(2, 0): (0, 0) if direct_x else (1, 0), (1, 0): (0, 0), (-1, 0): (0, 0)}
    for dx in (0, 1, -1, 2):
        for dz in (1, 2, 3):
            parent[dx, dz] = (dx, dz - 1)
            parent[dx, -dz] = (dx, 1 - dz)
        parent[dx, 4] = (dx, 3) if dx in (0, 1) else (dx, -3)
    return parent


def z_then_x(reach):
    parent = {}
    for far in (4, 3, -3, 2, -2, 1, -1):
        step = (abs(far) - 1) // reach * reach
        parent[0, far] = (0, step if far > 0 else -step)
    for dz in range(-3, 5):
        parent[1, dz] = (0, dz)
        parent[-1, dz] = (0, dz)
        parent[2, dz] = (1, dz) if dz % 2 == 0 else (-1, dz)
    return parent


TREES = {
    "wkv": z_then_x(4),
    "wq": x_then_z(True),
    "wo": z_then_x(1),
    "k": z_then_x(2),
    "v": x_then_z(False),
}
KB = {"wkv": 32, "wq": 64, "wo": 64, "k": 32, "v": 32}


def away(child, parent):
    dx = (child[0] - parent[0] + 1) % NX - 1
    dz = (child[1] - parent[1] + 3) % NZ - 3
    return dx, dz


def children_of(tree):
    below = {}
    for child, parent in tree.items():
        below.setdefault(parent, []).append(child)
    return below


def planned_steps():
    below = {g: children_of(t) for g, t in TREES.items()}
    free, heap, steps = {}, [], []
    got, tail = dict.fromkeys(TREES, 0), dict.fromkeys(TREES, 0.0)
    rows_in, waiting = {}, []
    now, hidden_left = 0.0, 6 * HALVES + 2
    keys_done = query_done = own_row_done = False

    def push(t, *what):
        heapq.heappush(heap, (round(t, 6), len(steps), len(heap), what))

    def transfer(route, kb, latency):
        end, hops = now, 0
        for link, n in route:
            free[link] = max(free.get(link, 0.0), now) + kb * n / RATE
            end, hops = max(end, free[link]), hops + n
        return end + latency + FURTHER * (hops - 1)

    push(0.0, "wkv", (0, 0))
    push(0.0, "wq", (0, 0))
    push(WO_START, "wo", (0, 0))
    for piece in range(HALVES):
        for sign in (1, -1):
            push(0.05, "hid", 0, sign, piece)
    while True:
        ahead = heap[0][0] if heap else math.inf
        keys_at = max(now, tail["wkv"] + HAND)
        query_at = max(now, tail["wq"] + HAND)
        if not keys_done and got["wkv"] == PLANE and not hidden_left and ahead >= keys_at - 0.3:
            now, keys_done = keys_at + 1.8, True
            steps.append(("keys",))
            push(now, "k", (0, 0))
            push(now + 0.01, "v", (0, 0))
            continue
        if keys_done and not query_done and got["wq"] == PLANE and ahead >= query_at - 0.3:
            now, query_done = query_at + 2.5, True
            steps.append(("query",))
            continue
        able = [w for w in waiting if own_row_done or w[1] == 0]
        if query_done and able and ahead >= max(now, able[0][0]) - 0.2:
            waiting.remove(able[0])
            now = max(now, able[0][0]) + 0.9
            own_row_done = True
            steps.append(("attend", able[0][1]))
            continue
        if not heap:
            return steps
        at, _, _, what = heapq.heappop(heap)
        now = max(now, at) + 0.03
        steps.append(what)
        if what[0] == "hid":
            _, hop, sign, piece = what
            if hop:
                hidden_left -= 1
                now += 0.25 / HALVES
            if hop < 3 or (hop == 3 and piece == (sign < 0)):
                route = [("y+" if sign > 0 else "y-", 1)]
                kb = TOK / HALVES
                push(transfer(route, kb, HOP_Y), "hid", hop + 1, sign, piece)
            continue
        g, o = what
        got[g] += 1
        tail[g] = max(tail[g], now)
        for child in below[g].get(o, ()):
            dx, dz = away(child, o)
            route = [("x+" if dx > 0 else "x-", abs(dx))] if dx else []
            route += [("z+" if dz > 0 else "z-", abs(dz))] if dz else []
            now += 0.03
            push(transfer(route, KB[g], HOP), g, child)
        now += 0.03
        if g in ("k", "v"):
            rows_in[o[1]] = rows_in.get(o[1], 0) + 1
            if rows_in[o[1]] == 2 * NX:
                waiting.append((now + HAND, o[1]))


class Gather:
    def __init__(self, tree, buf, arrive, handed, sent, place, by_row):
        self.below, self.buf, self.arrive = children_of(tree), buf, arrive
        self.handed, self.sent, self.place, self.by_row = handed, sent, place, by_row

    def index(self, o):
        z, x, c, y = self.place
        return (lax.rem(z - o[1] + NZ, NZ) * NX + lax.rem(x - o[0] + NX, NX)) * NC + c

    def slot(self, o):
        return (o[1] % NZ) * NX + o[0] % NX

    def to(self, src, device, sem):
        return pltpu.make_async_remote_copy(
            src_ref=src,
            dst_ref=src,
            send_sem=self.sent.at[0],
            recv_sem=sem,
            device_id=device,
            device_id_type=MESH_ID,
        )

    def arrived(self, o):
        z, x, c, y = self.place
        block = self.buf.at[self.index(o)]
        partner = (z, x, 1 - c, y)
        if o != (0, 0):
            self.to(block, partner, self.arrive.at[self.slot(o)]).wait_recv()
        for child in self.below.get(o, ()):
            dx, dz = away(child, o)
            near = (lax.rem(z + dz + NZ, NZ), lax.rem(x + dx + NX, NX), c, y)
            self.to(block, near, self.arrive.at[self.slot(child)]).start()
        row = o[1] % NZ if self.by_row else 0
        self.to(block, partner, self.handed.at[row]).start()

    def wait_handed(self, row=0):
        part = self.buf.at[pl.ds(0, NX if self.by_row else PLANE)]
        pltpu.make_async_copy(part, part, self.handed.at[row]).wait()

    def wait_sent(self):
        part = self.buf.at[pl.ds(0, BLOCKS - 1)]
        pltpu.make_async_copy(part, part, self.sent.at[0]).wait()


def kernel(
    hidden_ref,
    wq_ref,
    wkv_ref,
    wo_ref,
    span_ref,
    gain_ref,
    bq_ref,
    bkv_ref,
    inside_ref,
    spans_ref,
    mixed_ref,
    scale_ref,
    hid,
    gains,
    wkv,
    wq,
    wo,
    ks,
    vs,
    u,
    inv,
    rope,
    token_gap,
    qs,
    top,
    total,
    acc,
    attended,
    plus_in,
    minus_in,
    plus_out,
    minus_out,
    stats,
    local_sem,
    hid_arrive,
    hid_sent,
    gain_arrive,
    gain_sent,
    wkv_arrive,
    wkv_handed,
    wkv_sent,
    wq_arrive,
    wq_handed,
    wq_sent,
    wo_arrive,
    wo_handed,
    wo_sent,
    k_arrive,
    k_handed,
    k_sent,
    v_arrive,
    v_handed,
    v_sent,
    plus_arrive,
    plus_sent,
    minus_arrive,
    minus_sent,
    stats_arrive,
    stats_sent,
):
    z, x, c, y = (lax.axis_index(n) for n in ("z", "x", "c", "y"))
    place = (z, x, c, y)
    me = (z * NX + x) * NC + c

    def y_near(d):
        return (z, x, c, lax.rem(y + d + NY, NY))

    def y_at(d):
        return lax.rem(y + d + NY, NY)

    barrier = pltpu.get_barrier_semaphore()
    friends = [(z, x, 1 - c, y)]
    friends += [(lax.rem(z + d, NZ), x, c, y) for d in range(1, NZ)]
    friends += [(z, lax.rem(x + d, NX), c, y) for d in range(1, NX)]
    friends += [(z, x, c, lax.rem(y + d, NY)) for d in range(1, NY)]
    for f in friends:
        pl.semaphore_signal(barrier, inc=1, device_id=f, device_id_type=MESH_ID)
    starts = {
        "wkv": pltpu.make_async_copy(wkv_ref, wkv.at[me], local_sem.at[0]),
        "hid": pltpu.make_async_copy(hidden_ref, hid.at[y], local_sem.at[1]),
        "wq": pltpu.make_async_copy(wq_ref, wq.at[me], local_sem.at[2]),
        "wo": pltpu.make_async_copy(wo_ref, wo.at[me], local_sem.at[3]),
    }
    for s in starts.values():
        s.start()

    own_gain = gain_ref[...].astype(jnp.float32).reshape(1, COLS)
    gains[y] = jnp.broadcast_to(own_gain, (8, COLS))
    own_span = span_ref[me]
    of_span = spans_ref[own_span]
    cos_s, sin_s = of_span[0:1, :], of_span[1:2, :]
    rope[0] = inside_ref[0] * cos_s - inside_ref[1] * sin_s
    lanes = lax.broadcasted_iota(jnp.int32, (TOK, 128), 1)
    sine = inside_ref[1] * cos_s + inside_ref[0] * sin_s
    rope[1] = jnp.where(lanes < HEAD_SIZE // 2, -sine, sine)
    key_token = lax.broadcasted_iota(jnp.int32, (TOK, COLS), 0)
    query_token = lax.rem(lax.broadcasted_iota(jnp.int32, (TOK, COLS), 1), TOK)
    token_gap[...] = key_token - query_token
    inv[...] = jnp.zeros_like(inv)
    pl.semaphore_wait(barrier, len(friends))

    gathers = {
        "wkv": Gather(TREES["wkv"], wkv, wkv_arrive, wkv_handed, wkv_sent, place, False),
        "wq": Gather(TREES["wq"], wq, wq_arrive, wq_handed, wq_sent, place, False),
        "wo": Gather(TREES["wo"], wo, wo_arrive, wo_handed, wo_sent, place, False),
        "k": Gather(TREES["k"], ks, k_arrive, k_handed, k_sent, place, True),
        "v": Gather(TREES["v"], vs, v_arrive, v_handed, v_sent, place, True),
    }

    def remote(src, dst, sent, arrive, device):
        return pltpu.make_async_remote_copy(
            src_ref=src,
            dst_ref=dst,
            send_sem=sent,
            recv_sem=arrive,
            device_id=device,
            device_id_type=MESH_ID,
        )

    part_rows = TOK // HALVES

    def hid_copy(hop, sign, piece, arriving=False):
        source = y_at(-sign * (hop + 1 if arriving else hop))
        block = hid.at[source, pl.ds(piece * part_rows, part_rows)]
        k = (hop * HALVES + piece) * 2 + (sign > 0)
        return remote(block, block, hid_sent.at[k], hid_arrive.at[k], y_near(sign))

    def hid_goes(hop, sign, piece):
        return hop < 3 or (hop == 3 and piece == (sign < 0))

    def gain_copy(d, source):
        block = gains.at[source]
        return remote(block, block, gain_sent.at[d], gain_arrive.at[d], y_near(d))

    def prepare(source, piece):
        rows = slice(piece * part_rows, (piece + 1) * part_rows)
        h = hid[source, rows].astype(jnp.float32)
        u[source, rows] = (h * gains[source][0:1, :]).astype(jnp.bfloat16)
        squares = h * h
        part = squares[:, 0:128]
        for k in range(1, COLS // 128):
            part = part + squares[:, k * 128 : (k + 1) * 128]
        inv[rows] = inv[rows] + part

    def project(weights, width):
        def step(k, total):
            block = weights[pl.ds(k * (BLOCKS // NY), BLOCKS // NY)].reshape(COLS, width)
            return total + jnp.dot(u[k], block, preferred_element_type=jnp.float32)

        return lax.fori_loop(0, NY, step, jnp.zeros((TOK, width), jnp.float32))

    def rotate(head):
        return head * rope[0] + pltpu.roll(head, HEAD_SIZE // 2, 1) * rope[1]

    def make_keys():
        row_sum = jnp.sum(inv[...], axis=1, keepdims=True)
        inv[...] = jnp.broadcast_to(lax.rsqrt(row_sum / MODEL_WIDTH + eps), (TOK, 128))
        pair = project(wkv, 2 * HEAD_SIZE)
        scale = inv[...]
        keys = pair[:, :HEAD_SIZE] * scale + bkv_ref[0:1, :].astype(jnp.float32)
        values = pair[:, HEAD_SIZE:] * scale + bkv_ref[1:2, :].astype(jnp.float32)
        ks[me] = rotate(keys).astype(jnp.bfloat16)
        vs[me] = values.T.astype(jnp.bfloat16)

    def make_query():
        query = project(wq, COLS)
        bias = bq_ref[...].astype(jnp.float32).reshape(1, COLS)
        for g in range(GROUP):
            lanes = slice(g * HEAD_SIZE, (g + 1) * HEAD_SIZE)
            one = rotate(query[:, lanes] * inv[...] + bias[:, lanes])
            qs[g * TOK : (g + 1) * TOK, :] = one.astype(jnp.bfloat16)

    def attend(row):
        first = row == 0
        base = lax.rem(z - row + NZ, NZ) * NX * NC
        count = NX * NC
        keys = ks[pl.ds(base, count)].reshape(count * TOK, HEAD_SIZE)
        scores = lax.dot_general(
            keys, qs[...], (((1,), (1,)), ((), ())), preferred_element_type=jnp.float32
        )
        blocks, shifts, peak = [], [], None
        for k in range(count):
            block = scores[k * TOK : (k + 1) * TOK] * exponent_scale
            ahead = own_span - span_ref[base + k]
            if first:
                block = jnp.where(token_gap[...] <= ahead * TOK, block, -1e30)
                shift = jnp.float32(0.0)
            else:
                shift = jnp.where(ahead > 0, 0.0, 1e30).astype(jnp.float32)
            high = jnp.max(block, axis=0, keepdims=True) - shift
            peak = high if peak is None else jnp.maximum(peak, high)
            blocks.append(block)
            shifts.append(shift)
        if not first:
            old = top[0:1, :]
            peak = jnp.maximum(old, peak)
        weights, sums = [], None
        for block, shift in zip(blocks, shifts):
            w = jnp.exp2(block - (peak + shift))
            part = jnp.sum(w, axis=0, keepdims=True)
            sums = part if sums is None else sums + part
            weights.append(w.astype(jnp.bfloat16))
        values = jnp.concatenate([vs[base + k] for k in range(count)], axis=1)
        summed = jnp.dot(
            values, jnp.concatenate(weights, axis=0), preferred_element_type=jnp.float32
        )
        if not first:
            factor = jnp.exp2(old - peak)
            sums = sums + total[0:1, :] * factor
            summed = summed + acc[...] * factor
        top[0:1, :] = peak
        total[0:1, :] = sums
        acc[...] = summed

    seen_gain = {0}
    for step in planned_steps():
        if step[0] == "hid":
            _, hop, sign, piece = step
            if hop == 0:
                if piece == 0 and sign > 0:
                    starts["hid"].wait()
                hid_copy(0, sign, piece).start()
                if piece == HALVES - 1 and sign < 0:
                    for d in range(1, NY):
                        gain_copy(d, y).start()
                    for k in range(HALVES):
                        prepare(y, k)
            else:
                hid_copy(hop - 1, sign, piece, True).wait_recv()
                if hid_goes(hop, sign, piece):
                    hid_copy(hop, sign, piece).start()
                d = sign * hop % NY
                if d not in seen_gain:
                    seen_gain.add(d)
                    gain_copy(d, y_at(-d)).wait_recv()
                prepare(y_at(-d), piece)
        elif step[0] == "keys":
            gathers["wkv"].wait_handed()
            make_keys()
        elif step[0] == "query":
            gathers["wq"].wait_handed()
            make_query()
        elif step[0] == "attend":
            gathers["k"].wait_handed(step[1] % NZ)
            gathers["v"].wait_handed(step[1] % NZ)
            attend(step[1])
        else:
            g, o = step
            if o == (0, 0) and g in starts:
                starts[g].wait()
            gathers[g].arrived(o)
    for g in range(GROUP):
        lanes = slice(g * TOK, (g + 1) * TOK)
        one = (acc[:, lanes] / total[0:1, lanes]).T
        attended[:, g * HEAD_SIZE : (g + 1) * HEAD_SIZE] = one.astype(jnp.bfloat16)
    gathers["wo"].wait_handed()

    def partial(target):
        block = wo[pl.ds(target * (BLOCKS // NY), BLOCKS // NY)].reshape(COLS, COLS)
        return lax.dot_general(
            attended[...], block, (((1,), (1,)), ((), ())), preferred_element_type=jnp.float32
        )

    sub = TOK // SUBS
    half = COLS // 2

    def sum_copy(step, sign, piece):
        outs, ins, sent, arrive = (
            (plus_out, plus_in, plus_sent, plus_arrive)
            if sign > 0
            else (minus_out, minus_in, minus_sent, minus_arrive)
        )
        rows = pl.ds(piece * sub, sub)
        lanes = pl.ds(0, COLS)
        if step == 0:
            lanes = pl.ds(0 if sign > 0 else half, half)
        k = step * SUBS + piece
        return remote(
            outs.at[step, rows, lanes],
            ins.at[step, rows, lanes],
            sent.at[k],
            arrive.at[k],
            y_near(sign),
        )

    far = partial(y_at(4)).astype(jnp.bfloat16)
    plus_out[0, :, 0:half] = far[:, :half]
    minus_out[0, :, half:COLS] = far[:, half:]
    for piece in range(SUBS):
        sum_copy(0, 1, piece).start()
        sum_copy(0, -1, piece).start()
    for step in range(1, 4):
        terms = {1: partial(y_at(4 - step)), -1: partial(y_at(step - 4))}
        for piece in range(SUBS):
            rows = slice(piece * sub, (piece + 1) * sub)
            for sign in (1, -1):
                outs, ins = (plus_out, plus_in) if sign > 0 else (minus_out, minus_in)
                sum_copy(step - 1, sign, piece).wait_recv()
                term = terms[sign][rows]
                if step == 1:
                    lanes = slice(0, half) if sign > 0 else slice(half, COLS)
                    other = slice(half, COLS) if sign > 0 else slice(0, half)
                    got = ins[0, rows, lanes].astype(jnp.float32)
                    outs[1, rows, lanes] = (term[:, lanes] + got).astype(jnp.bfloat16)
                    outs[1, rows, other] = term[:, other].astype(jnp.bfloat16)
                else:
                    got = ins[step - 1, rows].astype(jnp.float32)
                    outs[step, rows] = (term + got).astype(jnp.bfloat16)
                sum_copy(step, sign, piece).start()
    own = partial(y)
    for piece in range(SUBS):
        rows = slice(piece * sub, (piece + 1) * sub)
        for sign in (1, -1):
            sum_copy(3, sign, piece).wait_recv()
        mixed = (
            own[rows]
            + plus_in[3, rows].astype(jnp.float32)
            + minus_in[3, rows].astype(jnp.float32)
        )
        mixed_ref[rows, :] = mixed
        stream = hid[y, rows].astype(jnp.float32) + mixed
        squares = stream * stream
        part = squares[:, 0:128]
        for k in range(1, COLS // 128):
            part = part + squares[:, k * 128 : (k + 1) * 128]
        inv[rows, :] = part

    column = jnp.sum(inv[...], axis=1, keepdims=True)
    stats[y] = jnp.broadcast_to(column, (TOK, 128)).T[0:8, :]

    def stats_copy(d, source):
        block = stats.at[source]
        return remote(block, block, stats_sent.at[d], stats_arrive.at[d], y_near(d))

    for d in range(1, NY):
        stats_copy(d, y).start()
    for g in gathers.values():
        g.wait_sent()
    for step in range(4):
        for sign in (1, -1):
            for piece in range(HALVES):
                if hid_goes(step, sign, piece):
                    hid_copy(step, sign, piece).wait_send()
            for piece in range(SUBS):
                sum_copy(step, sign, piece).wait_send()
    for d in range(1, NY):
        gain_copy(d, y).wait_send()
    for d in range(1, NY):
        stats_copy(d, y_at(-d)).wait_recv()
    summed = stats[0]
    for k in range(1, NY):
        summed = summed + stats[k]
    rows = jnp.broadcast_to(summed[0:1, :], (128, TOK)).T
    scale_ref[...] = lax.rsqrt(rows / MODEL_WIDTH + eps)
    for d in range(1, NY):
        stats_copy(d, y).wait_send()


def per_device(
    hidden_in,
    span_order,
    norm_gain,
    w_query,
    bias_query,
    key_value_weight,
    bias_kv,
    w_out,
    post_gain,
):
    half = HEAD_SIZE // 2
    inverse = rope_base ** (-(np.arange(HEAD_SIZE) % half) / half)
    row_angles = np.arange(TOK)[:, None] * inverse[None, :]
    span_angles = np.arange(BLOCKS)[:, None] * TOK * inverse[None, :]
    inside = np.stack([np.cos(row_angles), np.sin(row_angles)]).astype(np.float32)
    spans = np.stack([np.cos(span_angles), np.sin(span_angles)], axis=1).astype(np.float32)

    bf16, f32 = jnp.bfloat16, jnp.float32
    vmem = pl.BlockSpec(memory_space=pltpu.VMEM)
    smem = pl.BlockSpec(memory_space=pltpu.SMEM)
    anywhere = pl.BlockSpec(memory_space=pl.ANY)
    dma = pltpu.SemaphoreType.DMA
    gathers = []
    for rows in (1, 1, 1, NZ, NZ):
        gathers += [dma((PLANE,)), dma((rows,)), dma((1,))]
    mixed, scale = pl.pallas_call(
        kernel,
        out_shape=(
            jax.ShapeDtypeStruct((TOK, COLS), f32),
            jax.ShapeDtypeStruct((TOK, 128), f32),
        ),
        in_specs=[anywhere] * 4 + [smem] + [vmem] * 5,
        out_specs=(vmem, vmem),
        scratch_shapes=[
            pltpu.VMEM((NY, TOK, COLS), bf16),
            pltpu.VMEM((NY, 8, COLS), f32),
            pltpu.VMEM((BLOCKS, WROWS, 2 * HEAD_SIZE), bf16),
            pltpu.VMEM((BLOCKS, WROWS, COLS), bf16),
            pltpu.VMEM((BLOCKS, WROWS, COLS), bf16),
            pltpu.VMEM((BLOCKS, TOK, HEAD_SIZE), bf16),
            pltpu.VMEM((BLOCKS, TOK, HEAD_SIZE), bf16),
            pltpu.VMEM((NY, TOK, COLS), bf16),
            pltpu.VMEM((TOK, 128), f32),
            pltpu.VMEM((2, TOK, 128), f32),
            pltpu.VMEM((TOK, COLS), jnp.int32),
            pltpu.VMEM((COLS, HEAD_SIZE), bf16),
            pltpu.VMEM((8, COLS), f32),
            pltpu.VMEM((8, COLS), f32),
            pltpu.VMEM((HEAD_SIZE, COLS), f32),
            pltpu.VMEM((TOK, COLS), bf16),
            pltpu.VMEM((4, TOK, COLS), bf16),
            pltpu.VMEM((4, TOK, COLS), bf16),
            pltpu.VMEM((4, TOK, COLS), bf16),
            pltpu.VMEM((4, TOK, COLS), bf16),
            pltpu.VMEM((NY, 8, 128), f32),
            dma((4,)),
            dma((8 * HALVES,)),
            dma((8 * HALVES,)),
            dma((NY,)),
            dma((NY,)),
            *gathers,
            dma((4 * SUBS,)),
            dma((4 * SUBS,)),
            dma((4 * SUBS,)),
            dma((4 * SUBS,)),
            dma((NY,)),
            dma((NY,)),
        ],
        compiler_params=pltpu.CompilerParams(
            collective_id=0, has_side_effects=True, vmem_limit_bytes=56 << 20
        ),
    )(
        hidden_in,
        w_query,
        key_value_weight.reshape(WROWS, 2 * HEAD_SIZE),
        w_out.T,
        span_order,
        norm_gain,
        bias_query,
        bias_kv,
        jnp.asarray(inside),
        jnp.asarray(spans),
    )
    stream = hidden_in.astype(f32) + mixed
    normed = stream * scale[:, 0:1] * post_gain.astype(f32)[None, :]
    return mixed.astype(bf16), normed.astype(bf16)


def solution(mesh):
    torus = Mesh(mesh.devices.reshape(NZ, NX, NC, NY), ("z", "x", "c", "y"))
    in_specs = (
        P(SEQ, "y"),
        P(),
        P("y"),
        P(SEQ, "y"),
        P("y"),
        P(SEQ, None, "y"),
        P(None, "y"),
        P("y", SEQ),
        P("y"),
    )
    out_specs = (P(SEQ, "y"), P(SEQ, "y"))
    return jax.shard_map(
        per_device, mesh=torus, in_specs=in_specs, out_specs=out_specs, check_vma=False
    )
```

```python
import heapq
import math

import jax
import jax.numpy as jnp
import numpy as np
from jax import lax
from jax.experimental import pallas as pl
from jax.experimental.pallas import tpu as pltpu
from jax.sharding import Mesh
from jax.sharding import PartitionSpec as P

MODEL_WIDTH = 4096
HEAD_SIZE = 128
GROUP = 4
TOK = 128
NZ, NX, NC, NY = 8, 4, 2, 8
PLANE = NZ * NX
BLOCKS = PLANE * NC
COLS = MODEL_WIDTH // NY
WROWS = MODEL_WIDTH // BLOCKS
SUBS = 4
HALVES = 2
SEQ = ("z", "x", "c")
MESH_ID = pl.DeviceIdType.MESH

eps = 1e-06
rope_base = 1000000.0
exponent_scale = math.log2(math.e) / math.sqrt(HEAD_SIZE)

RATE, HOP, FURTHER, HOP_Y, HAND = 46.6, 3.3, 0.7, 2.1, 1.6
WO_START = 12.0


def x_then_z(direct_x):
    parent = {(2, 0): (0, 0) if direct_x else (1, 0), (1, 0): (0, 0), (-1, 0): (0, 0)}
    for dx in (0, 1, -1, 2):
        for dz in (1, 2, 3):
            parent[dx, dz] = (dx, dz - 1)
            parent[dx, -dz] = (dx, 1 - dz)
        parent[dx, 4] = (dx, 3) if dx in (0, 1) else (dx, -3)
    return parent


def z_then_x(reach):
    parent = {}
    for far in (4, 3, -3, 2, -2, 1, -1):
        step = (abs(far) - 1) // reach * reach
        parent[0, far] = (0, step if far > 0 else -step)
    for dz in range(-3, 5):
        parent[1, dz] = (0, dz)
        parent[-1, dz] = (0, dz)
        parent[2, dz] = (1, dz) if dz % 2 == 0 else (-1, dz)
    return parent


TREES = {
    "wkv": z_then_x(4),
    "wq": x_then_z(True),
    "wo": z_then_x(1),
    "k": z_then_x(2),
    "v": x_then_z(False),
}
KB = {"wkv": 32, "wq": 64, "wo": 64, "k": 32, "v": 32}


def away(child, parent):
    dx = (child[0] - parent[0] + 1) % NX - 1
    dz = (child[1] - parent[1] + 3) % NZ - 3
    return dx, dz


def children_of(tree):
    below = {}
    for child, parent in tree.items():
        below.setdefault(parent, []).append(child)
    return below


def planned_steps():
    below = {g: children_of(t) for g, t in TREES.items()}
    free, heap, steps = {}, [], []
    got, tail = dict.fromkeys(TREES, 0), dict.fromkeys(TREES, 0.0)
    rows_in, waiting = {}, []
    now, hidden_left = 0.0, 6 * HALVES + 2
    keys_done = query_done = own_row_done = False

    def push(t, *what):
        heapq.heappush(heap, (round(t, 6), len(steps), len(heap), what))

    def transfer(route, kb, latency):
        end, hops = now, 0
        for link, n in route:
            free[link] = max(free.get(link, 0.0), now) + kb * n / RATE
            end, hops = max(end, free[link]), hops + n
        return end + latency + FURTHER * (hops - 1)

    push(0.0, "wkv", (0, 0))
    push(0.0, "wq", (0, 0))
    push(WO_START, "wo", (0, 0))
    for piece in range(HALVES):
        for sign in (1, -1):
            push(0.05, "hid", 0, sign, piece)
    while True:
        ahead = heap[0][0] if heap else math.inf
        keys_at = max(now, tail["wkv"] + HAND)
        query_at = max(now, tail["wq"] + HAND)
        if not keys_done and got["wkv"] == PLANE and not hidden_left and ahead >= keys_at - 0.3:
            now, keys_done = keys_at + 1.8, True
            steps.append(("keys",))
            push(now, "k", (0, 0))
            push(now + 0.01, "v", (0, 0))
            continue
        if keys_done and not query_done and got["wq"] == PLANE and ahead >= query_at - 0.3:
            now, query_done = query_at + 2.5, True
            steps.append(("query",))
            continue
        able = [w for w in waiting if own_row_done or w[1] == 0]
        if query_done and able and ahead >= max(now, able[0][0]) - 0.2:
            waiting.remove(able[0])
            now = max(now, able[0][0]) + 0.9
            own_row_done = True
            steps.append(("attend", able[0][1]))
            continue
        if not heap:
            return steps
        at, _, _, what = heapq.heappop(heap)
        now = max(now, at) + 0.03
        steps.append(what)
        if what[0] == "hid":
            _, hop, sign, piece = what
            if hop:
                hidden_left -= 1
                now += 0.25 / HALVES
            if hop < 3 or (hop == 3 and piece == (sign < 0)):
                route = [("y+" if sign > 0 else "y-", 1)]
                kb = TOK / HALVES
                push(transfer(route, kb, HOP_Y), "hid", hop + 1, sign, piece)
            continue
        g, o = what
        got[g] += 1
        tail[g] = max(tail[g], now)
        for child in below[g].get(o, ()):
            dx, dz = away(child, o)
            route = [("x+" if dx > 0 else "x-", abs(dx))] if dx else []
            route += [("z+" if dz > 0 else "z-", abs(dz))] if dz else []
            now += 0.03
            push(transfer(route, KB[g], HOP), g, child)
        now += 0.03
        if g in ("k", "v"):
            rows_in[o[1]] = rows_in.get(o[1], 0) + 1
            if rows_in[o[1]] == 2 * NX:
                waiting.append((now + HAND, o[1]))


class Gather:
    def __init__(self, tree, buf, arrive, handed, sent, place, by_row):
        self.below, self.buf, self.arrive = children_of(tree), buf, arrive
        self.handed, self.sent, self.place, self.by_row = handed, sent, place, by_row

    def index(self, o):
        z, x, c, y = self.place
        return (lax.rem(z - o[1] + NZ, NZ) * NX + lax.rem(x - o[0] + NX, NX)) * NC + c

    def slot(self, o):
        return (o[1] % NZ) * NX + o[0] % NX

    def to(self, src, device, sem):
        return pltpu.make_async_remote_copy(
            src_ref=src,
            dst_ref=src,
            send_sem=self.sent.at[0],
            recv_sem=sem,
            device_id=device,
            device_id_type=MESH_ID,
        )

    def arrived(self, o):
        z, x, c, y = self.place
        block = self.buf.at[self.index(o)]
        partner = (z, x, 1 - c, y)
        if o != (0, 0):
            self.to(block, partner, self.arrive.at[self.slot(o)]).wait_recv()
        for child in self.below.get(o, ()):
            dx, dz = away(child, o)
            near = (lax.rem(z + dz + NZ, NZ), lax.rem(x + dx + NX, NX), c, y)
            self.to(block, near, self.arrive.at[self.slot(child)]).start()
        row = o[1] % NZ if self.by_row else 0
        self.to(block, partner, self.handed.at[row]).start()

    def wait_handed(self, row=0):
        part = self.buf.at[pl.ds(0, NX if self.by_row else PLANE)]
        pltpu.make_async_copy(part, part, self.handed.at[row]).wait()

    def wait_sent(self):
        part = self.buf.at[pl.ds(0, BLOCKS - 1)]
        pltpu.make_async_copy(part, part, self.sent.at[0]).wait()


def kernel(
    hidden_in_hbm,
    wq_hbm,
    wkv_hbm,
    wo_hbm,
    span_hbm,
    gain_hbm,
    bq_hbm,
    bkv_hbm,
    post_hbm,
    inside_hbm,
    spans_hbm,
    mixed_ref,
    normed_ref,
    pair_weight,
    span_ref,
    gain_ref,
    bq_ref,
    bkv_ref,
    post_ref,
    inside_ref,
    spans_ref,
    hid,
    gains,
    wkv,
    wq,
    wo,
    ks,
    vs,
    u,
    inv,
    rope,
    token_gap,
    qs,
    top,
    total,
    acc,
    attended,
    plus_in,
    minus_in,
    plus_out,
    minus_out,
    stats,
    local_sem,
    hid_arrive,
    hid_sent,
    gain_arrive,
    gain_sent,
    wkv_arrive,
    wkv_handed,
    wkv_sent,
    wq_arrive,
    wq_handed,
    wq_sent,
    wo_arrive,
    wo_handed,
    wo_sent,
    k_arrive,
    k_handed,
    k_sent,
    v_arrive,
    v_handed,
    v_sent,
    plus_arrive,
    plus_sent,
    minus_arrive,
    minus_sent,
    stats_arrive,
    stats_sent,
):
    z, x, c, y = (lax.axis_index(n) for n in ("z", "x", "c", "y"))
    place = (z, x, c, y)
    me = (z * NX + x) * NC + c

    def y_near(d):
        return (z, x, c, lax.rem(y + d + NY, NY))

    def y_at(d):
        return lax.rem(y + d + NY, NY)

    barrier = pltpu.get_barrier_semaphore()
    friends = [(z, x, 1 - c, y)]
    friends += [(lax.rem(z + d, NZ), x, c, y) for d in range(1, NZ)]
    friends += [(z, lax.rem(x + d, NX), c, y) for d in range(1, NX)]
    friends += [(z, x, c, lax.rem(y + d, NY)) for d in range(1, NY)]
    for f in friends:
        pl.semaphore_signal(barrier, inc=1, device_id=f, device_id_type=MESH_ID)
    starts = {}
    for name, src, dst in (
        ("wkv", wkv_hbm, pair_weight),
        ("span", span_hbm, span_ref),
        ("gain", gain_hbm, gain_ref),
        ("inside", inside_hbm, inside_ref),
        ("spans", spans_hbm, spans_ref),
        ("hid", hidden_in_hbm, hid.at[y]),
        ("wq", wq_hbm, wq.at[me]),
        ("bkv", bkv_hbm, bkv_ref),
        ("bq", bq_hbm, bq_ref),
        ("wo", wo_hbm, wo.at[me]),
        ("post", post_hbm, post_ref),
    ):
        starts[name] = pltpu.make_async_copy(src, dst, local_sem.at[len(starts)])
        starts[name].start()

    starts["wkv"].wait()
    wkv[me, :, 0:HEAD_SIZE] = pair_weight[:, 0, :]
    wkv[me, :, HEAD_SIZE : 2 * HEAD_SIZE] = pair_weight[:, 1, :]
    for name in ("span", "gain", "inside", "spans", "bkv", "bq", "post"):
        starts[name].wait()
    own_gain = gain_ref[...].astype(jnp.float32).reshape(1, COLS)
    gains[y] = jnp.broadcast_to(own_gain, (8, COLS))
    own_span = span_ref[me]
    of_span = spans_ref[own_span]
    cos_s, sin_s = of_span[0:1, :], of_span[1:2, :]
    rope[0] = inside_ref[0] * cos_s - inside_ref[1] * sin_s
    lanes = lax.broadcasted_iota(jnp.int32, (TOK, 128), 1)
    sine = inside_ref[1] * cos_s + inside_ref[0] * sin_s
    rope[1] = jnp.where(lanes < HEAD_SIZE // 2, -sine, sine)
    key_token = lax.broadcasted_iota(jnp.int32, (TOK, COLS), 0)
    query_token = lax.rem(lax.broadcasted_iota(jnp.int32, (TOK, COLS), 1), TOK)
    token_gap[...] = key_token - query_token
    inv[...] = jnp.zeros_like(inv)
    pl.semaphore_wait(barrier, len(friends))

    gathers = {
        "wkv": Gather(TREES["wkv"], wkv, wkv_arrive, wkv_handed, wkv_sent, place, False),
        "wq": Gather(TREES["wq"], wq, wq_arrive, wq_handed, wq_sent, place, False),
        "wo": Gather(TREES["wo"], wo, wo_arrive, wo_handed, wo_sent, place, False),
        "k": Gather(TREES["k"], ks, k_arrive, k_handed, k_sent, place, True),
        "v": Gather(TREES["v"], vs, v_arrive, v_handed, v_sent, place, True),
    }

    def remote(src, dst, sent, arrive, device):
        return pltpu.make_async_remote_copy(
            src_ref=src,
            dst_ref=dst,
            send_sem=sent,
            recv_sem=arrive,
            device_id=device,
            device_id_type=MESH_ID,
        )

    part_rows = TOK // HALVES

    def hid_copy(hop, sign, piece, arriving=False):
        source = y_at(-sign * (hop + 1 if arriving else hop))
        block = hid.at[source, pl.ds(piece * part_rows, part_rows)]
        k = (hop * HALVES + piece) * 2 + (sign > 0)
        return remote(block, block, hid_sent.at[k], hid_arrive.at[k], y_near(sign))

    def hid_goes(hop, sign, piece):
        return hop < 3 or (hop == 3 and piece == (sign < 0))

    def gain_copy(d, source):
        block = gains.at[source]
        return remote(block, block, gain_sent.at[d], gain_arrive.at[d], y_near(d))

    def prepare(source, piece):
        rows = slice(piece * part_rows, (piece + 1) * part_rows)
        h = hid[source, rows].astype(jnp.float32)
        u[source, rows] = (h * gains[source][0:1, :]).astype(jnp.bfloat16)
        squares = h * h
        part = squares[:, 0:128]
        for k in range(1, COLS // 128):
            part = part + squares[:, k * 128 : (k + 1) * 128]
        inv[rows] = inv[rows] + part

    def project(weights, width):
        def step(k, total):
            block = weights[pl.ds(k * (BLOCKS // NY), BLOCKS // NY)].reshape(COLS, width)
            return total + jnp.dot(u[k], block, preferred_element_type=jnp.float32)

        return lax.fori_loop(0, NY, step, jnp.zeros((TOK, width), jnp.float32))

    def rotate(head):
        return head * rope[0] + pltpu.roll(head, HEAD_SIZE // 2, 1) * rope[1]

    def make_keys():
        row_sum = jnp.sum(inv[...], axis=1, keepdims=True)
        inv[...] = jnp.broadcast_to(lax.rsqrt(row_sum / MODEL_WIDTH + eps), (TOK, 128))
        pair = project(wkv, 2 * HEAD_SIZE)
        scale = inv[...]
        keys = pair[:, :HEAD_SIZE] * scale + bkv_ref[0:1, :].astype(jnp.float32)
        values = pair[:, HEAD_SIZE:] * scale + bkv_ref[1:2, :].astype(jnp.float32)
        ks[me] = rotate(keys).astype(jnp.bfloat16)
        vs[me] = values.T.astype(jnp.bfloat16)

    def make_query():
        query = project(wq, COLS)
        bias = bq_ref[...].astype(jnp.float32).reshape(1, COLS)
        for g in range(GROUP):
            lanes = slice(g * HEAD_SIZE, (g + 1) * HEAD_SIZE)
            one = rotate(query[:, lanes] * inv[...] + bias[:, lanes])
            qs[g * TOK : (g + 1) * TOK, :] = one.astype(jnp.bfloat16)

    def attend(row):
        first = row == 0
        base = lax.rem(z - row + NZ, NZ) * NX * NC
        count = NX * NC
        keys = ks[pl.ds(base, count)].reshape(count * TOK, HEAD_SIZE)
        scores = lax.dot_general(
            keys, qs[...], (((1,), (1,)), ((), ())), preferred_element_type=jnp.float32
        )
        blocks, shifts, peak = [], [], None
        for k in range(count):
            block = scores[k * TOK : (k + 1) * TOK] * exponent_scale
            ahead = own_span - span_ref[base + k]
            if first:
                block = jnp.where(token_gap[...] <= ahead * TOK, block, -1e30)
                shift = jnp.float32(0.0)
            else:
                shift = jnp.where(ahead > 0, 0.0, 1e30).astype(jnp.float32)
            high = jnp.max(block, axis=0, keepdims=True) - shift
            peak = high if peak is None else jnp.maximum(peak, high)
            blocks.append(block)
            shifts.append(shift)
        if not first:
            old = top[0:1, :]
            peak = jnp.maximum(old, peak)
        weights, sums = [], None
        for block, shift in zip(blocks, shifts):
            w = jnp.exp2(block - (peak + shift))
            part = jnp.sum(w, axis=0, keepdims=True)
            sums = part if sums is None else sums + part
            weights.append(w.astype(jnp.bfloat16))
        values = jnp.concatenate([vs[base + k] for k in range(count)], axis=1)
        summed = jnp.dot(
            values, jnp.concatenate(weights, axis=0), preferred_element_type=jnp.float32
        )
        if not first:
            factor = jnp.exp2(old - peak)
            sums = sums + total[0:1, :] * factor
            summed = summed + acc[...] * factor
        top[0:1, :] = peak
        total[0:1, :] = sums
        acc[...] = summed

    seen_gain = {0}
    for step in planned_steps():
        if step[0] == "hid":
            _, hop, sign, piece = step
            if hop == 0:
                if piece == 0 and sign > 0:
                    starts["hid"].wait()
                hid_copy(0, sign, piece).start()
                if piece == HALVES - 1 and sign < 0:
                    for d in range(1, NY):
                        gain_copy(d, y).start()
                    for k in range(HALVES):
                        prepare(y, k)
            else:
                hid_copy(hop - 1, sign, piece, True).wait_recv()
                if hid_goes(hop, sign, piece):
                    hid_copy(hop, sign, piece).start()
                d = sign * hop % NY
                if d not in seen_gain:
                    seen_gain.add(d)
                    gain_copy(d, y_at(-d)).wait_recv()
                prepare(y_at(-d), piece)
        elif step[0] == "keys":
            gathers["wkv"].wait_handed()
            make_keys()
        elif step[0] == "query":
            gathers["wq"].wait_handed()
            make_query()
        elif step[0] == "attend":
            gathers["k"].wait_handed(step[1] % NZ)
            gathers["v"].wait_handed(step[1] % NZ)
            attend(step[1])
        else:
            g, o = step
            if o == (0, 0) and g in ("wq", "wo"):
                starts[g].wait()
            gathers[g].arrived(o)
    for g in range(GROUP):
        lanes = slice(g * TOK, (g + 1) * TOK)
        one = (acc[:, lanes] / total[0:1, lanes]).T
        attended[:, g * HEAD_SIZE : (g + 1) * HEAD_SIZE] = one.astype(jnp.bfloat16)
    gathers["wo"].wait_handed()

    def partial(target):
        block = wo[pl.ds(target * (BLOCKS // NY), BLOCKS // NY)].reshape(COLS, COLS)
        return lax.dot_general(
            attended[...], block, (((1,), (1,)), ((), ())), preferred_element_type=jnp.float32
        )

    sub = TOK // SUBS
    half = COLS // 2

    def sum_copy(step, sign, piece):
        outs, ins, sent, arrive = (
            (plus_out, plus_in, plus_sent, plus_arrive)
            if sign > 0
            else (minus_out, minus_in, minus_sent, minus_arrive)
        )
        rows = pl.ds(piece * sub, sub)
        lanes = pl.ds(0, COLS)
        if step == 0:
            lanes = pl.ds(0 if sign > 0 else half, half)
        k = step * SUBS + piece
        return remote(
            outs.at[step, rows, lanes],
            ins.at[step, rows, lanes],
            sent.at[k],
            arrive.at[k],
            y_near(sign),
        )

    far = partial(y_at(4)).astype(jnp.bfloat16)
    plus_out[0, :, 0:half] = far[:, :half]
    minus_out[0, :, half:COLS] = far[:, half:]
    for piece in range(SUBS):
        sum_copy(0, 1, piece).start()
        sum_copy(0, -1, piece).start()
    for step in range(1, 4):
        terms = {1: partial(y_at(4 - step)), -1: partial(y_at(step - 4))}
        for piece in range(SUBS):
            rows = slice(piece * sub, (piece + 1) * sub)
            for sign in (1, -1):
                outs, ins = (plus_out, plus_in) if sign > 0 else (minus_out, minus_in)
                sum_copy(step - 1, sign, piece).wait_recv()
                term = terms[sign][rows]
                if step == 1:
                    lanes = slice(0, half) if sign > 0 else slice(half, COLS)
                    other = slice(half, COLS) if sign > 0 else slice(0, half)
                    got = ins[0, rows, lanes].astype(jnp.float32)
                    outs[1, rows, lanes] = (term[:, lanes] + got).astype(jnp.bfloat16)
                    outs[1, rows, other] = term[:, other].astype(jnp.bfloat16)
                else:
                    got = ins[step - 1, rows].astype(jnp.float32)
                    outs[step, rows] = (term + got).astype(jnp.bfloat16)
                sum_copy(step, sign, piece).start()
    own = partial(y)
    for piece in range(SUBS):
        rows = slice(piece * sub, (piece + 1) * sub)
        for sign in (1, -1):
            sum_copy(3, sign, piece).wait_recv()
        mixed = (
            own[rows]
            + plus_in[3, rows].astype(jnp.float32)
            + minus_in[3, rows].astype(jnp.float32)
        )
        mixed_ref[rows, :] = mixed
        stream = hid[y, rows].astype(jnp.float32) + mixed
        squares = stream * stream
        part = squares[:, 0:128]
        for k in range(1, COLS // 128):
            part = part + squares[:, k * 128 : (k + 1) * 128]
        inv[rows, :] = part

    column = jnp.sum(inv[...], axis=1, keepdims=True)
    stats[y] = jnp.broadcast_to(column, (TOK, 128)).T[0:8, :]

    def stats_copy(d, source):
        block = stats.at[source]
        return remote(block, block, stats_sent.at[d], stats_arrive.at[d], y_near(d))

    for d in range(1, NY):
        stats_copy(d, y).start()
    for g in gathers.values():
        g.wait_sent()
    for step in range(4):
        for sign in (1, -1):
            for piece in range(HALVES):
                if hid_goes(step, sign, piece):
                    hid_copy(step, sign, piece).wait_send()
            for piece in range(SUBS):
                sum_copy(step, sign, piece).wait_send()
    for d in range(1, NY):
        gain_copy(d, y).wait_send()
    for d in range(1, NY):
        stats_copy(d, y_at(-d)).wait_recv()
    summed = stats[0]
    for k in range(1, NY):
        summed = summed + stats[k]
    rows = jnp.broadcast_to(summed[0:1, :], (128, TOK)).T
    scale = lax.rsqrt(rows / MODEL_WIDTH + eps)
    post = post_ref[...].astype(jnp.float32).reshape(1, COLS)
    for g in range(GROUP):
        lanes = slice(g * 128, (g + 1) * 128)
        stream = hid[y, :, lanes].astype(jnp.float32) + mixed_ref[:, lanes]
        normed_ref[:, lanes] = stream * scale * post[:, lanes]
    for d in range(1, NY):
        stats_copy(d, y).wait_send()


def per_device(
    hidden_in,
    span_order,
    norm_gain,
    w_query,
    bias_query,
    key_value_weight,
    bias_kv,
    w_out,
    post_gain,
):
    half = HEAD_SIZE // 2
    inverse = rope_base ** (-(np.arange(HEAD_SIZE) % half) / half)
    row_angles = np.arange(TOK)[:, None] * inverse[None, :]
    span_angles = np.arange(BLOCKS)[:, None] * TOK * inverse[None, :]
    inside = np.stack([np.cos(row_angles), np.sin(row_angles)]).astype(np.float32)
    spans = np.stack([np.cos(span_angles), np.sin(span_angles)], axis=1).astype(np.float32)

    bf16, f32 = jnp.bfloat16, jnp.float32
    vmem = pl.BlockSpec(memory_space=pltpu.VMEM)
    anywhere = pl.BlockSpec(memory_space=pl.ANY)
    dma = pltpu.SemaphoreType.DMA
    gathers = []
    for rows in (1, 1, 1, NZ, NZ):
        gathers += [dma((PLANE,)), dma((rows,)), dma((1,))]
    mixed, normed = pl.pallas_call(
        kernel,
        out_shape=(
            jax.ShapeDtypeStruct((TOK, COLS), f32),
            jax.ShapeDtypeStruct((TOK, COLS), f32),
        ),
        in_specs=[anywhere] * 11,
        out_specs=(vmem, vmem),
        scratch_shapes=[
            pltpu.VMEM((WROWS, 2, HEAD_SIZE), bf16),
            pltpu.SMEM((BLOCKS,), jnp.int32),
            pltpu.VMEM((COLS,), bf16),
            pltpu.VMEM((COLS,), bf16),
            pltpu.VMEM((2, HEAD_SIZE), bf16),
            pltpu.VMEM((COLS,), bf16),
            pltpu.VMEM((2, TOK, HEAD_SIZE), f32),
            pltpu.VMEM((BLOCKS, 2, HEAD_SIZE), f32),
            pltpu.VMEM((NY, TOK, COLS), bf16),
            pltpu.VMEM((NY, 8, COLS), f32),
            pltpu.VMEM((BLOCKS, WROWS, 2 * HEAD_SIZE), bf16),
            pltpu.VMEM((BLOCKS, WROWS, COLS), bf16),
            pltpu.VMEM((BLOCKS, WROWS, COLS), bf16),
            pltpu.VMEM((BLOCKS, TOK, HEAD_SIZE), bf16),
            pltpu.VMEM((BLOCKS, TOK, HEAD_SIZE), bf16),
            pltpu.VMEM((NY, TOK, COLS), bf16),
            pltpu.VMEM((TOK, 128), f32),
            pltpu.VMEM((2, TOK, 128), f32),
            pltpu.VMEM((TOK, COLS), jnp.int32),
            pltpu.VMEM((COLS, HEAD_SIZE), bf16),
            pltpu.VMEM((8, COLS), f32),
            pltpu.VMEM((8, COLS), f32),
            pltpu.VMEM((HEAD_SIZE, COLS), f32),
            pltpu.VMEM((TOK, COLS), bf16),
            pltpu.VMEM((4, TOK, COLS), bf16),
            pltpu.VMEM((4, TOK, COLS), bf16),
            pltpu.VMEM((4, TOK, COLS), bf16),
            pltpu.VMEM((4, TOK, COLS), bf16),
            pltpu.VMEM((NY, 8, 128), f32),
            dma((11,)),
            dma((8 * HALVES,)),
            dma((8 * HALVES,)),
            dma((NY,)),
            dma((NY,)),
            *gathers,
            dma((4 * SUBS,)),
            dma((4 * SUBS,)),
            dma((4 * SUBS,)),
            dma((4 * SUBS,)),
            dma((NY,)),
            dma((NY,)),
        ],
        compiler_params=pltpu.CompilerParams(
            collective_id=0, has_side_effects=True, vmem_limit_bytes=56 << 20
        ),
    )(
        hidden_in,
        w_query,
        key_value_weight,
        w_out.T,
        span_order,
        norm_gain,
        bias_query,
        bias_kv,
        post_gain,
        jnp.asarray(inside),
        jnp.asarray(spans),
    )
    return mixed.astype(bf16), normed.astype(bf16)


def solution(mesh):
    torus = Mesh(mesh.devices.reshape(NZ, NX, NC, NY), ("z", "x", "c", "y"))
    in_specs = (
        P(SEQ, "y"),
        P(),
        P("y"),
        P(SEQ, "y"),
        P("y"),
        P(SEQ, None, "y"),
        P(None, "y"),
        P("y", SEQ),
        P("y"),
    )
    out_specs = (P(SEQ, "y"), P(SEQ, "y"))
    return jax.shard_map(
        per_device, mesh=torus, in_specs=in_specs, out_specs=out_specs, check_vma=False
    )
```

```python
import heapq
import math

import jax
import jax.numpy as jnp
import numpy as np
from jax import lax
from jax.experimental import pallas as pl
from jax.experimental.pallas import tpu as pltpu
from jax.sharding import Mesh
from jax.sharding import PartitionSpec as P

MODEL_WIDTH = 4096
HEAD_SIZE = 128
GROUP = 4
TOK = 128
NZ, NX, NC, NY = 8, 4, 2, 8
PLANE = NZ * NX
BLOCKS = PLANE * NC
COLS = MODEL_WIDTH // NY
WROWS = MODEL_WIDTH // BLOCKS
SUBS = 4
HALVES = 2
SEQ = ("z", "x", "c")
MESH_ID = pl.DeviceIdType.MESH

eps = 1e-06
rope_base = 1000000.0
exponent_scale = math.log2(math.e) / math.sqrt(HEAD_SIZE)

RATE, HOP, FURTHER, HOP_Y, HAND = 46.6, 2.2, 0.7, 2.1, 1.6
WQ_START, WO_START = 0.0, 0.0


def x_then_z(direct_x):
    parent = {(2, 0): (0, 0) if direct_x else (1, 0), (1, 0): (0, 0), (-1, 0): (0, 0)}
    for dx in (0, 1, -1, 2):
        for dz in (1, 2, 3):
            parent[dx, dz] = (dx, dz - 1)
            parent[dx, -dz] = (dx, 1 - dz)
        parent[dx, 4] = (dx, 3) if dx in (0, 1) else (dx, -3)
    return parent


def z_then_x(reach):
    parent = {}
    for far in (4, 3, -3, 2, -2, 1, -1):
        step = (abs(far) - 1) // reach * reach
        parent[0, far] = (0, step if far > 0 else -step)
    for dz in range(-3, 5):
        parent[1, dz] = (0, dz)
        parent[-1, dz] = (0, dz)
        parent[2, dz] = (1, dz) if dz % 2 == 0 else (-1, dz)
    return parent


def mirrored(tree):
    def turn(o):
        return (o[0] if o[0] == NX // 2 else -o[0], o[1] if o[1] == NZ // 2 else -o[1])

    return {turn(child): turn(parent) for child, parent in tree.items()}


TREES = {
    "wkv": mirrored(z_then_x(3)),
    "wq": mirrored(z_then_x(1)),
    "wo": mirrored(x_then_z(True)),
    "k": mirrored(x_then_z(True)),
    "v": mirrored(z_then_x(2)),
}
KB = {"wkv": 32, "wq": 64, "wo": 64, "k": 32, "v": 32}


def away(child, parent):
    dx = (child[0] - parent[0] + 1) % NX - 1
    dz = (child[1] - parent[1] + 3) % NZ - 3
    return dx, dz


def children_of(tree):
    below = {}
    for child, parent in tree.items():
        below.setdefault(parent, []).append(child)
    return below


def planned_steps():
    below = {g: children_of(t) for g, t in TREES.items()}
    free, heap, steps = {}, [], []
    got, tail = dict.fromkeys(TREES, 0), dict.fromkeys(TREES, 0.0)
    rows_in, waiting = {}, []
    now, hidden_left = 0.0, 7 * HALVES
    keys_done = query_done = own_row_done = False

    def push(t, *what):
        heapq.heappush(heap, (round(t, 6), len(steps), len(heap), what))

    def transfer(route, kb, latency):
        end, hops = now, 0
        for link, n in route:
            free[link] = max(free.get(link, 0.0), now) + kb * n / RATE
            end, hops = max(end, free[link]), hops + n
        return end + latency + FURTHER * (hops - 1)

    push(0.0, "wkv", (0, 0))
    push(WQ_START, "wq", (0, 0))
    push(WO_START, "wo", (0, 0))
    for piece in range(HALVES):
        for sign in (1, -1):
            push(0.05, "hid", 0, sign, piece)
    while True:
        ahead = heap[0][0] if heap else math.inf
        keys_at = max(now, tail["wkv"] + HAND)
        query_at = max(now, tail["wq"] + HAND)
        if not keys_done and got["wkv"] == PLANE and not hidden_left and ahead >= keys_at - 0.3:
            now, keys_done = keys_at + 1.8, True
            steps.append(("keys",))
            push(now, "k", (0, 0))
            push(now + 0.01, "v", (0, 0))
            continue
        if keys_done and not query_done and got["wq"] == PLANE and ahead >= query_at - 0.3:
            now, query_done = query_at + 2.5, True
            steps.append(("query",))
            continue
        able = [w for w in waiting if own_row_done or w[1] == 0]
        if query_done and able and ahead >= max(now, able[0][0]) - 0.2:
            waiting.remove(able[0])
            now = max(now, able[0][0]) + 0.9
            own_row_done = True
            steps.append(("attend", able[0][1]))
            continue
        if not heap:
            return steps
        at, _, _, what = heapq.heappop(heap)
        now = max(now, at) + 0.03
        steps.append(what)
        if what[0] == "hid":
            _, hop, sign, piece = what
            if hop:
                hidden_left -= 1
                now += 0.25 / HALVES
            if hop < 3 or (hop == 3 and (piece < HALVES // 2) == (sign > 0)):
                route = [("y+" if sign > 0 else "y-", 1)]
                kb = TOK / HALVES
                push(transfer(route, kb, HOP_Y), "hid", hop + 1, sign, piece)
            continue
        g, o = what
        got[g] += 1
        tail[g] = max(tail[g], now)
        for child in below[g].get(o, ()):
            dx, dz = away(child, o)
            route = [("x+" if dx > 0 else "x-", abs(dx))] if dx else []
            route += [("z+" if dz > 0 else "z-", abs(dz))] if dz else []
            now += 0.03
            push(transfer(route, KB[g], HOP), g, child)
        now += 0.03
        if g in ("k", "v"):
            rows_in[o[1]] = rows_in.get(o[1], 0) + 1
            if rows_in[o[1]] == 2 * NX:
                waiting.append((now + HAND, o[1]))


class Gather:
    def __init__(self, tree, buf, arrive, handed, sent, place, by_row):
        self.below, self.buf, self.arrive = children_of(tree), buf, arrive
        self.handed, self.sent, self.place, self.by_row = handed, sent, place, by_row

    def index(self, o):
        z, x, c, y = self.place
        return (lax.rem(z - o[1] + NZ, NZ) * NX + lax.rem(x - o[0] + NX, NX)) * NC + c

    def slot(self, o):
        return (o[1] % NZ) * NX + o[0] % NX

    def to(self, src, device, sem):
        return pltpu.make_async_remote_copy(
            src_ref=src,
            dst_ref=src,
            send_sem=self.sent.at[0],
            recv_sem=sem,
            device_id=device,
            device_id_type=MESH_ID,
        )

    def arrived(self, o):
        z, x, c, y = self.place
        block = self.buf.at[self.index(o)]
        partner = (z, x, 1 - c, y)
        if o != (0, 0):
            self.to(block, partner, self.arrive.at[self.slot(o)]).wait_recv()
        for child in self.below.get(o, ()):
            dx, dz = away(child, o)
            near = (lax.rem(z + dz + NZ, NZ), lax.rem(x + dx + NX, NX), c, y)
            self.to(block, near, self.arrive.at[self.slot(child)]).start()
        row = o[1] % NZ if self.by_row else 0
        self.to(block, partner, self.handed.at[row]).start()

    def wait_handed(self, row=0):
        part = self.buf.at[pl.ds(0, NX if self.by_row else PLANE)]
        pltpu.make_async_copy(part, part, self.handed.at[row]).wait()

    def wait_sent(self):
        part = self.buf.at[pl.ds(0, BLOCKS - 1)]
        pltpu.make_async_copy(part, part, self.sent.at[0]).wait()


def kernel(
    hidden_in_hbm,
    wq_hbm,
    wkv_hbm,
    wo_hbm,
    span_hbm,
    gain_hbm,
    bq_hbm,
    bkv_hbm,
    post_hbm,
    inside_hbm,
    spans_hbm,
    both_ref,
    mixed_ref,
    pair_weight,
    span_ref,
    gain_ref,
    bq_ref,
    bkv_ref,
    post_ref,
    inside_ref,
    spans_ref,
    hid,
    gains,
    wkv,
    wq,
    wo,
    ks,
    vs,
    u,
    inv,
    rope,
    token_gap,
    qs,
    top,
    total,
    acc,
    attended,
    plus_in,
    minus_in,
    plus_out,
    minus_out,
    stats,
    local_sem,
    hid_arrive,
    hid_sent,
    gain_arrive,
    gain_sent,
    wkv_arrive,
    wkv_handed,
    wkv_sent,
    wq_arrive,
    wq_handed,
    wq_sent,
    wo_arrive,
    wo_handed,
    wo_sent,
    k_arrive,
    k_handed,
    k_sent,
    v_arrive,
    v_handed,
    v_sent,
    plus_arrive,
    plus_sent,
    minus_arrive,
    minus_sent,
    stats_arrive,
    stats_sent,
):
    z, x, c, y = (lax.axis_index(n) for n in ("z", "x", "c", "y"))
    place = (z, x, c, y)
    me = (z * NX + x) * NC + c

    def y_near(d):
        return (z, x, c, lax.rem(y + d + NY, NY))

    def y_at(d):
        return lax.rem(y + d + NY, NY)

    barrier = pltpu.get_barrier_semaphore()
    friends = [(z, x, 1 - c, y)]
    friends += [(lax.rem(z + d, NZ), x, c, y) for d in range(1, NZ)]
    friends += [(z, lax.rem(x + d, NX), c, y) for d in range(1, NX)]
    friends += [(z, x, c, lax.rem(y + d, NY)) for d in range(1, NY)]
    for f in friends:
        pl.semaphore_signal(barrier, inc=1, device_id=f, device_id_type=MESH_ID)
    starts = {}
    for name, src, dst in (
        ("wkv", wkv_hbm, pair_weight),
        ("span", span_hbm, span_ref),
        ("gain", gain_hbm, gain_ref),
        ("inside", inside_hbm, inside_ref),
        ("spans", spans_hbm, spans_ref),
        ("hid", hidden_in_hbm, hid.at[y]),
        ("wq", wq_hbm, wq.at[me]),
        ("bkv", bkv_hbm, bkv_ref),
        ("bq", bq_hbm, bq_ref),
        ("wo", wo_hbm, wo.at[me]),
        ("post", post_hbm, post_ref),
    ):
        starts[name] = pltpu.make_async_copy(src, dst, local_sem.at[len(starts)])
        starts[name].start()

    starts["wkv"].wait()
    wkv[me, :, 0:HEAD_SIZE] = pair_weight[:, 0, :]
    wkv[me, :, HEAD_SIZE : 2 * HEAD_SIZE] = pair_weight[:, 1, :]
    for name in ("span", "gain", "inside", "spans", "bkv", "bq", "post"):
        starts[name].wait()
    own_gain = gain_ref[...].astype(jnp.float32).reshape(1, COLS)
    gains[y] = jnp.broadcast_to(own_gain, (8, COLS))
    own_span = span_ref[me]
    of_span = spans_ref[own_span]
    cos_s, sin_s = of_span[0:1, :], of_span[1:2, :]
    rope[0] = inside_ref[0] * cos_s - inside_ref[1] * sin_s
    lanes = lax.broadcasted_iota(jnp.int32, (TOK, 128), 1)
    sine = inside_ref[1] * cos_s + inside_ref[0] * sin_s
    rope[1] = jnp.where(lanes < HEAD_SIZE // 2, -sine, sine)
    key_token = lax.broadcasted_iota(jnp.int32, (TOK, COLS), 0)
    query_token = lax.rem(lax.broadcasted_iota(jnp.int32, (TOK, COLS), 1), TOK)
    token_gap[...] = key_token - query_token
    inv[...] = jnp.zeros_like(inv)
    pl.semaphore_wait(barrier, len(friends))

    gathers = {
        "wkv": Gather(TREES["wkv"], wkv, wkv_arrive, wkv_handed, wkv_sent, place, False),
        "wq": Gather(TREES["wq"], wq, wq_arrive, wq_handed, wq_sent, place, False),
        "wo": Gather(TREES["wo"], wo, wo_arrive, wo_handed, wo_sent, place, False),
        "k": Gather(TREES["k"], ks, k_arrive, k_handed, k_sent, place, True),
        "v": Gather(TREES["v"], vs, v_arrive, v_handed, v_sent, place, True),
    }

    def remote(src, dst, sent, arrive, device):
        return pltpu.make_async_remote_copy(
            src_ref=src,
            dst_ref=dst,
            send_sem=sent,
            recv_sem=arrive,
            device_id=device,
            device_id_type=MESH_ID,
        )

    part_rows = TOK // HALVES

    def hid_copy(hop, sign, piece, arriving=False):
        source = y_at(-sign * (hop + 1 if arriving else hop))
        block = hid.at[source, pl.ds(piece * part_rows, part_rows)]
        k = (hop * HALVES + piece) * 2 + (sign > 0)
        return remote(block, block, hid_sent.at[k], hid_arrive.at[k], y_near(sign))

    def hid_goes(hop, sign, piece):
        return hop < 3 or (hop == 3 and (piece < HALVES // 2) == (sign > 0))

    def gain_copy(d, source):
        block = gains.at[source]
        return remote(block, block, gain_sent.at[d], gain_arrive.at[d], y_near(d))

    def prepare(source, piece):
        rows = slice(piece * part_rows, (piece + 1) * part_rows)
        h = hid[source, rows].astype(jnp.float32)
        u[source, rows] = (h * gains[source][0:1, :]).astype(jnp.bfloat16)
        squares = h * h
        part = squares[:, 0:128]
        for k in range(1, COLS // 128):
            part = part + squares[:, k * 128 : (k + 1) * 128]
        inv[rows] = inv[rows] + part

    def project(weights, width):
        def step(k, total):
            block = weights[pl.ds(k * (BLOCKS // NY), BLOCKS // NY)].reshape(COLS, width)
            return total + jnp.dot(u[k], block, preferred_element_type=jnp.float32)

        zero = jnp.zeros((TOK, width), jnp.float32)
        return lax.fori_loop(0, NY, step, zero, unroll=True)

    def rotate(head):
        return head * rope[0] + pltpu.roll(head, HEAD_SIZE // 2, 1) * rope[1]

    def make_keys():
        row_sum = jnp.sum(inv[...], axis=1, keepdims=True)
        inv[...] = jnp.broadcast_to(lax.rsqrt(row_sum / MODEL_WIDTH + eps), (TOK, 128))
        pair = project(wkv, 2 * HEAD_SIZE)
        scale = inv[...]
        keys = pair[:, :HEAD_SIZE] * scale + bkv_ref[0:1, :].astype(jnp.float32)
        values = pair[:, HEAD_SIZE:] * scale + bkv_ref[1:2, :].astype(jnp.float32)
        ks[me] = rotate(keys).astype(jnp.bfloat16)
        vs[me] = values.T.astype(jnp.bfloat16)

    def make_query():
        query = project(wq, COLS)
        bias = bq_ref[...].astype(jnp.float32).reshape(1, COLS)
        for g in range(GROUP):
            lanes = slice(g * HEAD_SIZE, (g + 1) * HEAD_SIZE)
            one = rotate(query[:, lanes] * inv[...] + bias[:, lanes])
            qs[g * TOK : (g + 1) * TOK, :] = one.astype(jnp.bfloat16)

    def attend(row):
        first = row == 0
        base = lax.rem(z - row + NZ, NZ) * NX * NC
        count = NX * NC
        keys = ks[pl.ds(base, count)].reshape(count * TOK, HEAD_SIZE)
        scores = lax.dot_general(
            keys, qs[...], (((1,), (1,)), ((), ())), preferred_element_type=jnp.float32
        )
        blocks, shifts, peak = [], [], None
        for k in range(count):
            block = scores[k * TOK : (k + 1) * TOK] * exponent_scale
            ahead = own_span - span_ref[base + k]
            if first:
                block = jnp.where(token_gap[...] <= ahead * TOK, block, -1e30)
                shift = jnp.float32(0.0)
            else:
                shift = jnp.where(ahead > 0, 0.0, 1e30).astype(jnp.float32)
            high = jnp.max(block, axis=0, keepdims=True) - shift
            peak = high if peak is None else jnp.maximum(peak, high)
            blocks.append(block)
            shifts.append(shift)
        if not first:
            old = top[0:1, :]
            peak = jnp.maximum(old, peak)
        weights, sums = [], None
        for block, shift in zip(blocks, shifts):
            w = jnp.exp2(block - (peak + shift))
            part = jnp.sum(w, axis=0, keepdims=True)
            sums = part if sums is None else sums + part
            weights.append(w.astype(jnp.bfloat16))
        values = jnp.concatenate([vs[base + k] for k in range(count)], axis=1)
        summed = jnp.dot(
            values, jnp.concatenate(weights, axis=0), preferred_element_type=jnp.float32
        )
        if not first:
            factor = jnp.exp2(old - peak)
            sums = sums + total[0:1, :] * factor
            summed = summed + acc[...] * factor
        top[0:1, :] = peak
        total[0:1, :] = sums
        acc[...] = summed

    seen_gain = {0}
    for step in planned_steps():
        if step[0] == "hid":
            _, hop, sign, piece = step
            if hop == 0:
                if piece == 0 and sign > 0:
                    starts["hid"].wait()
                hid_copy(0, sign, piece).start()
                if piece == HALVES - 1 and sign < 0:
                    for d in range(1, NY):
                        gain_copy(d, y).start()
                    for k in range(HALVES):
                        prepare(y, k)
            else:
                hid_copy(hop - 1, sign, piece, True).wait_recv()
                if hid_goes(hop, sign, piece):
                    hid_copy(hop, sign, piece).start()
                d = sign * hop % NY
                if d not in seen_gain:
                    seen_gain.add(d)
                    gain_copy(d, y_at(-d)).wait_recv()
                prepare(y_at(-d), piece)
        elif step[0] == "keys":
            gathers["wkv"].wait_handed()
            make_keys()
        elif step[0] == "query":
            gathers["wq"].wait_handed()
            make_query()
        elif step[0] == "attend":
            gathers["k"].wait_handed(step[1] % NZ)
            gathers["v"].wait_handed(step[1] % NZ)
            attend(step[1])
        else:
            g, o = step
            if o == (0, 0) and g in ("wq", "wo"):
                starts[g].wait()
            gathers[g].arrived(o)
    for g in range(GROUP):
        lanes = slice(g * TOK, (g + 1) * TOK)
        one = (acc[:, lanes] / total[0:1, lanes]).T
        attended[:, g * HEAD_SIZE : (g + 1) * HEAD_SIZE] = one.astype(jnp.bfloat16)
    gathers["wo"].wait_handed()

    def partial(target):
        block = wo[pl.ds(target * (BLOCKS // NY), BLOCKS // NY)].reshape(COLS, COLS)
        return lax.dot_general(
            attended[...], block, (((1,), (1,)), ((), ())), preferred_element_type=jnp.float32
        )

    sub = TOK // SUBS
    half = COLS // 2

    def sum_copy(step, sign, piece):
        outs, ins, sent, arrive = (
            (plus_out, plus_in, plus_sent, plus_arrive)
            if sign > 0
            else (minus_out, minus_in, minus_sent, minus_arrive)
        )
        rows = pl.ds(piece * sub, sub)
        lanes = pl.ds(0, COLS)
        if step == 0:
            lanes = pl.ds(0 if sign > 0 else half, half)
        k = step * SUBS + piece
        return remote(
            outs.at[step, rows, lanes],
            ins.at[step, rows, lanes],
            sent.at[k],
            arrive.at[k],
            y_near(sign),
        )

    far = partial(y_at(4)).astype(jnp.bfloat16)
    plus_out[0, :, 0:half] = far[:, :half]
    minus_out[0, :, half:COLS] = far[:, half:]
    for piece in range(SUBS):
        sum_copy(0, 1, piece).start()
        sum_copy(0, -1, piece).start()
    for step in range(1, 4):
        terms = {1: partial(y_at(4 - step)), -1: partial(y_at(step - 4))}
        for piece in range(SUBS):
            rows = slice(piece * sub, (piece + 1) * sub)
            for sign in (1, -1):
                outs, ins = (plus_out, plus_in) if sign > 0 else (minus_out, minus_in)
                sum_copy(step - 1, sign, piece).wait_recv()
                term = terms[sign][rows]
                if step == 1:
                    lanes = slice(0, half) if sign > 0 else slice(half, COLS)
                    other = slice(half, COLS) if sign > 0 else slice(0, half)
                    got = ins[0, rows, lanes].astype(jnp.float32)
                    outs[1, rows, lanes] = (term[:, lanes] + got).astype(jnp.bfloat16)
                    outs[1, rows, other] = term[:, other].astype(jnp.bfloat16)
                else:
                    got = ins[step - 1, rows].astype(jnp.float32)
                    outs[step, rows] = (term + got).astype(jnp.bfloat16)
                sum_copy(step, sign, piece).start()
    own = partial(y)
    for piece in range(SUBS):
        rows = slice(piece * sub, (piece + 1) * sub)
        for sign in (1, -1):
            sum_copy(3, sign, piece).wait_recv()
        mixed = (
            own[rows]
            + plus_in[3, rows].astype(jnp.float32)
            + minus_in[3, rows].astype(jnp.float32)
        )
        mixed_ref[rows, :] = mixed
        both_ref[0, rows, :] = mixed.astype(jnp.bfloat16)
        stream = hid[y, rows].astype(jnp.float32) + mixed
        squares = stream * stream
        part = squares[:, 0:128]
        for k in range(1, COLS // 128):
            part = part + squares[:, k * 128 : (k + 1) * 128]
        inv[rows, :] = part

    column = jnp.sum(inv[...], axis=1, keepdims=True)
    stats[y] = jnp.broadcast_to(column, (TOK, 128)).T[0:8, :]

    def stats_copy(d, source):
        block = stats.at[source]
        return remote(block, block, stats_sent.at[d], stats_arrive.at[d], y_near(d))

    for d in range(1, NY):
        stats_copy(d, y).start()
    for g in gathers.values():
        g.wait_sent()
    for step in range(4):
        for sign in (1, -1):
            for piece in range(HALVES):
                if hid_goes(step, sign, piece):
                    hid_copy(step, sign, piece).wait_send()
            for piece in range(SUBS):
                sum_copy(step, sign, piece).wait_send()
    for d in range(1, NY):
        gain_copy(d, y).wait_send()
    for d in range(1, NY):
        stats_copy(d, y_at(-d)).wait_recv()
    summed = stats[0]
    for k in range(1, NY):
        summed = summed + stats[k]
    rows = jnp.broadcast_to(summed[0:1, :], (128, TOK)).T
    scale = lax.rsqrt(rows / MODEL_WIDTH + eps)
    post = post_ref[...].astype(jnp.float32).reshape(1, COLS)
    for g in range(GROUP):
        lanes = slice(g * 128, (g + 1) * 128)
        stream = hid[y, :, lanes].astype(jnp.float32) + mixed_ref[:, lanes]
        both_ref[1, :, lanes] = (stream * scale * post[:, lanes]).astype(jnp.bfloat16)
    for d in range(1, NY):
        stats_copy(d, y).wait_send()


def per_device(
    hidden_in,
    span_order,
    norm_gain,
    w_query,
    bias_query,
    key_value_weight,
    bias_kv,
    w_out,
    post_gain,
):
    half = HEAD_SIZE // 2
    inverse = rope_base ** (-(np.arange(HEAD_SIZE) % half) / half)
    row_angles = np.arange(TOK)[:, None] * inverse[None, :]
    span_angles = np.arange(BLOCKS)[:, None] * TOK * inverse[None, :]
    inside = np.stack([np.cos(row_angles), np.sin(row_angles)]).astype(np.float32)
    spans = np.stack([np.cos(span_angles), np.sin(span_angles)], axis=1).astype(np.float32)

    bf16, f32 = jnp.bfloat16, jnp.float32
    vmem = pl.BlockSpec(memory_space=pltpu.VMEM)
    anywhere = pl.BlockSpec(memory_space=pl.ANY)
    dma = pltpu.SemaphoreType.DMA
    gathers = []
    for rows in (1, 1, 1, NZ, NZ):
        gathers += [dma((PLANE,)), dma((rows,)), dma((1,))]
    both = pl.pallas_call(
        kernel,
        out_shape=jax.ShapeDtypeStruct((2, TOK, COLS), bf16),
        in_specs=[anywhere] * 11,
        out_specs=vmem,
        scratch_shapes=[
            pltpu.VMEM((TOK, COLS), f32),
            pltpu.VMEM((WROWS, 2, HEAD_SIZE), bf16),
            pltpu.SMEM((BLOCKS,), jnp.int32),
            pltpu.VMEM((COLS,), bf16),
            pltpu.VMEM((COLS,), bf16),
            pltpu.VMEM((2, HEAD_SIZE), bf16),
            pltpu.VMEM((COLS,), bf16),
            pltpu.VMEM((2, TOK, HEAD_SIZE), f32),
            pltpu.VMEM((BLOCKS, 2, HEAD_SIZE), f32),
            pltpu.VMEM((NY, TOK, COLS), bf16),
            pltpu.VMEM((NY, 8, COLS), f32),
            pltpu.VMEM((BLOCKS, WROWS, 2 * HEAD_SIZE), bf16),
            pltpu.VMEM((BLOCKS, WROWS, COLS), bf16),
            pltpu.VMEM((BLOCKS, WROWS, COLS), bf16),
            pltpu.VMEM((BLOCKS, TOK, HEAD_SIZE), bf16),
            pltpu.VMEM((BLOCKS, TOK, HEAD_SIZE), bf16),
            pltpu.VMEM((NY, TOK, COLS), bf16),
            pltpu.VMEM((TOK, 128), f32),
            pltpu.VMEM((2, TOK, 128), f32),
            pltpu.VMEM((TOK, COLS), jnp.int32),
            pltpu.VMEM((COLS, HEAD_SIZE), bf16),
            pltpu.VMEM((8, COLS), f32),
            pltpu.VMEM((8, COLS), f32),
            pltpu.VMEM((HEAD_SIZE, COLS), f32),
            pltpu.VMEM((TOK, COLS), bf16),
            pltpu.VMEM((4, TOK, COLS), bf16),
            pltpu.VMEM((4, TOK, COLS), bf16),
            pltpu.VMEM((4, TOK, COLS), bf16),
            pltpu.VMEM((4, TOK, COLS), bf16),
            pltpu.VMEM((NY, 8, 128), f32),
            dma((11,)),
            dma((8 * HALVES,)),
            dma((8 * HALVES,)),
            dma((NY,)),
            dma((NY,)),
            *gathers,
            dma((4 * SUBS,)),
            dma((4 * SUBS,)),
            dma((4 * SUBS,)),
            dma((4 * SUBS,)),
            dma((NY,)),
            dma((NY,)),
        ],
        compiler_params=pltpu.CompilerParams(
            collective_id=0, has_side_effects=True, vmem_limit_bytes=56 << 20
        ),
    )(
        hidden_in,
        w_query,
        key_value_weight,
        w_out.T,
        span_order,
        norm_gain,
        bias_query,
        bias_kv,
        post_gain,
        jnp.asarray(inside),
        jnp.asarray(spans),
    )
    return both[0], both[1]


def solution(mesh):
    torus = Mesh(mesh.devices.reshape(NZ, NX, NC, NY), ("z", "x", "c", "y"))
    in_specs = (
        P(SEQ, "y"),
        P(),
        P("y"),
        P(SEQ, "y"),
        P("y"),
        P(SEQ, None, "y"),
        P(None, "y"),
        P("y", SEQ),
        P("y"),
    )
    out_specs = (P(SEQ, "y"), P(SEQ, "y"))
    return jax.shard_map(
        per_device, mesh=torus, in_specs=in_specs, out_specs=out_specs, check_vma=False
    )
```

```python
import heapq
import math

import jax
import jax.numpy as jnp
import numpy as np
from jax import lax
from jax.experimental import pallas as pl
from jax.experimental.pallas import tpu as pltpu
from jax.sharding import Mesh
from jax.sharding import PartitionSpec as P

MODEL_WIDTH = 4096
HEAD_SIZE = 128
GROUP = 4
TOK = 128
NZ, NX, NC, NY = 8, 4, 2, 8
PLANE = NZ * NX
BLOCKS = PLANE * NC
COLS = MODEL_WIDTH // NY
WROWS = MODEL_WIDTH // BLOCKS
SUBS = 4
HALVES = 2
SEQ = ("z", "x", "c")
MESH_ID = pl.DeviceIdType.MESH

eps = 1e-06
rope_base = 1000000.0
exponent_scale = math.log2(math.e) / math.sqrt(HEAD_SIZE)

RATE, HOP, FURTHER, HOP_Y, HAND = 46.6, 2.2, 0.7, 2.1, 1.6
WQ_START, WO_START = 0.0, 0.0


def x_then_z(direct_x):
    parent = {(2, 0): (0, 0) if direct_x else (1, 0), (1, 0): (0, 0), (-1, 0): (0, 0)}
    for dx in (0, 1, -1, 2):
        for dz in (1, 2, 3):
            parent[dx, dz] = (dx, dz - 1)
            parent[dx, -dz] = (dx, 1 - dz)
        parent[dx, 4] = (dx, 3) if dx in (0, 1) else (dx, -3)
    return parent


def z_then_x(reach):
    parent = {}
    for far in (4, 3, -3, 2, -2, 1, -1):
        step = (abs(far) - 1) // reach * reach
        parent[0, far] = (0, step if far > 0 else -step)
    for dz in range(-3, 5):
        parent[1, dz] = (0, dz)
        parent[-1, dz] = (0, dz)
        parent[2, dz] = (1, dz) if dz % 2 == 0 else (-1, dz)
    return parent


def mirrored(tree):
    def turn(o):
        return (o[0] if o[0] == NX // 2 else -o[0], o[1] if o[1] == NZ // 2 else -o[1])

    return {turn(child): turn(parent) for child, parent in tree.items()}


TREES = {
    "wkv": mirrored(z_then_x(3)),
    "wq": mirrored(z_then_x(1)),
    "wo": mirrored(x_then_z(True)),
    "k": mirrored(x_then_z(True)),
    "v": mirrored(z_then_x(2)),
}
KB = {"wkv": 32, "wq": 64, "wo": 64, "k": 32, "v": 32}


def away(child, parent):
    dx = (child[0] - parent[0] + 1) % NX - 1
    dz = (child[1] - parent[1] + 3) % NZ - 3
    return dx, dz


def children_of(tree):
    below = {}
    for child, parent in tree.items():
        below.setdefault(parent, []).append(child)
    return below


def planned_steps():
    below = {g: children_of(t) for g, t in TREES.items()}
    free, heap, steps = {}, [], []
    got, tail = dict.fromkeys(TREES, 0), dict.fromkeys(TREES, 0.0)
    rows_in, waiting = {}, []
    now, hidden_left = 0.0, 7 * HALVES
    keys_done = query_done = own_row_done = False

    def push(t, *what):
        heapq.heappush(heap, (round(t, 6), len(steps), len(heap), what))

    def transfer(route, kb, latency):
        end, hops = now, 0
        for link, n in route:
            free[link] = max(free.get(link, 0.0), now) + kb * n / RATE
            end, hops = max(end, free[link]), hops + n
        return end + latency + FURTHER * (hops - 1)

    push(0.0, "wkv", (0, 0))
    push(WQ_START, "wq", (0, 0))
    push(WO_START, "wo", (0, 0))
    for piece in range(HALVES):
        for sign in (1, -1):
            push(0.05, "hid", 0, sign, piece)
    while True:
        ahead = heap[0][0] if heap else math.inf
        keys_at = max(now, tail["wkv"] + HAND)
        query_at = max(now, tail["wq"] + HAND)
        if not keys_done and got["wkv"] == PLANE and not hidden_left and ahead >= keys_at - 0.3:
            now, keys_done = keys_at + 1.1, True
            steps.append(("keys",))
            push(now, "k", (0, 0))
            push(now + 0.01, "v", (0, 0))
            continue
        if keys_done and not query_done and got["wq"] == PLANE and ahead >= query_at - 0.3:
            now, query_done = query_at + 1.5, True
            steps.append(("query",))
            continue
        able = [w for w in waiting if own_row_done or w[1] == 0]
        if query_done and able and ahead >= max(now, able[0][0]) - 0.2:
            waiting.remove(able[0])
            now = max(now, able[0][0]) + 0.7
            own_row_done = True
            steps.append(("attend", able[0][1]))
            continue
        if not heap:
            return steps
        at, _, _, what = heapq.heappop(heap)
        now = max(now, at) + 0.03
        steps.append(what)
        if what[0] == "hid":
            _, hop, sign, piece = what
            if hop:
                hidden_left -= 1
                now += 0.25 / HALVES
            if hop < 3 or (hop == 3 and (piece < HALVES // 2) == (sign > 0)):
                route = [("y+" if sign > 0 else "y-", 1)]
                kb = TOK / HALVES
                push(transfer(route, kb, HOP_Y), "hid", hop + 1, sign, piece)
            continue
        g, o = what
        got[g] += 1
        tail[g] = max(tail[g], now)
        for child in below[g].get(o, ()):
            dx, dz = away(child, o)
            route = [("x+" if dx > 0 else "x-", abs(dx))] if dx else []
            route += [("z+" if dz > 0 else "z-", abs(dz))] if dz else []
            now += 0.03
            push(transfer(route, KB[g], HOP), g, child)
        now += 0.03
        if g in ("k", "v"):
            rows_in[o[1]] = rows_in.get(o[1], 0) + 1
            if rows_in[o[1]] == 2 * NX:
                waiting.append((now + HAND, o[1]))


class Gather:
    def __init__(self, tree, buf, arrive, handed, sent, place, by_row):
        self.below, self.buf, self.arrive = children_of(tree), buf, arrive
        self.handed, self.sent, self.place, self.by_row = handed, sent, place, by_row

    def index(self, o):
        z, x, c, y = self.place
        return (lax.rem(z - o[1] + NZ, NZ) * NX + lax.rem(x - o[0] + NX, NX)) * NC + c

    def slot(self, o):
        return (o[1] % NZ) * NX + o[0] % NX

    def to(self, src, device, sem):
        return pltpu.make_async_remote_copy(
            src_ref=src,
            dst_ref=src,
            send_sem=self.sent.at[0],
            recv_sem=sem,
            device_id=device,
            device_id_type=MESH_ID,
        )

    def arrived(self, o):
        z, x, c, y = self.place
        block = self.buf.at[self.index(o)]
        partner = (z, x, 1 - c, y)
        if o != (0, 0):
            self.to(block, partner, self.arrive.at[self.slot(o)]).wait_recv()
        for child in self.below.get(o, ()):
            dx, dz = away(child, o)
            near = (lax.rem(z + dz + NZ, NZ), lax.rem(x + dx + NX, NX), c, y)
            self.to(block, near, self.arrive.at[self.slot(child)]).start()
        row = o[1] % NZ if self.by_row else 0
        self.to(block, partner, self.handed.at[row]).start()

    def wait_handed(self, row=0):
        part = self.buf.at[pl.ds(0, NX if self.by_row else PLANE)]
        pltpu.make_async_copy(part, part, self.handed.at[row]).wait()

    def wait_sent(self):
        part = self.buf.at[pl.ds(0, BLOCKS - 1)]
        pltpu.make_async_copy(part, part, self.sent.at[0]).wait()


def kernel(
    hidden_in_hbm,
    wq_hbm,
    wkv_hbm,
    wo_hbm,
    span_hbm,
    gain_hbm,
    bq_hbm,
    bkv_hbm,
    post_hbm,
    inside_hbm,
    spans_hbm,
    both_ref,
    mixed_ref,
    pair_weight,
    span_ref,
    gain_ref,
    bq_ref,
    bkv_ref,
    post_ref,
    inside_ref,
    spans_ref,
    hid,
    gains,
    wkv,
    wq,
    wo,
    ks,
    vs,
    u,
    inv,
    rope,
    token_gap,
    qs,
    top,
    total,
    acc,
    attended,
    plus_in,
    minus_in,
    plus_out,
    minus_out,
    stats,
    local_sem,
    hid_arrive,
    hid_sent,
    gain_arrive,
    gain_sent,
    wkv_arrive,
    wkv_handed,
    wkv_sent,
    wq_arrive,
    wq_handed,
    wq_sent,
    wo_arrive,
    wo_handed,
    wo_sent,
    k_arrive,
    k_handed,
    k_sent,
    v_arrive,
    v_handed,
    v_sent,
    plus_arrive,
    plus_sent,
    minus_arrive,
    minus_sent,
    stats_arrive,
    stats_sent,
):
    z, x, c, y = (lax.axis_index(n) for n in ("z", "x", "c", "y"))
    place = (z, x, c, y)
    me = (z * NX + x) * NC + c

    def y_near(d):
        return (z, x, c, lax.rem(y + d + NY, NY))

    def y_at(d):
        return lax.rem(y + d + NY, NY)

    barrier = pltpu.get_barrier_semaphore()
    friends = [(z, x, 1 - c, y)]
    friends += [(lax.rem(z + d, NZ), x, c, y) for d in range(1, NZ)]
    friends += [(z, lax.rem(x + d, NX), c, y) for d in range(1, NX)]
    friends += [(z, x, c, lax.rem(y + d, NY)) for d in range(1, NY)]
    for f in friends:
        pl.semaphore_signal(barrier, inc=1, device_id=f, device_id_type=MESH_ID)
    starts = {}
    for name, src, dst in (
        ("wkv", wkv_hbm, pair_weight),
        ("span", span_hbm, span_ref),
        ("gain", gain_hbm, gain_ref),
        ("inside", inside_hbm, inside_ref),
        ("spans", spans_hbm, spans_ref),
        ("hid", hidden_in_hbm, hid.at[y]),
        ("wq", wq_hbm, wq.at[me]),
        ("bkv", bkv_hbm, bkv_ref),
        ("bq", bq_hbm, bq_ref),
        ("wo", wo_hbm, wo.at[me]),
        ("post", post_hbm, post_ref),
    ):
        starts[name] = pltpu.make_async_copy(src, dst, local_sem.at[len(starts)])
        starts[name].start()

    starts["wkv"].wait()
    wkv[me, :, 0:HEAD_SIZE] = pair_weight[:, 0, :]
    wkv[me, :, HEAD_SIZE : 2 * HEAD_SIZE] = pair_weight[:, 1, :]
    for name in ("span", "gain", "inside", "spans", "bkv", "bq", "post"):
        starts[name].wait()
    own_gain = gain_ref[...].astype(jnp.float32).reshape(1, COLS)
    gains[y] = jnp.broadcast_to(own_gain, (8, COLS))
    own_span = span_ref[me]
    of_span = spans_ref[own_span]
    cos_s, sin_s = of_span[0:1, :], of_span[1:2, :]
    rope[0] = inside_ref[0] * cos_s - inside_ref[1] * sin_s
    lanes = lax.broadcasted_iota(jnp.int32, (TOK, 128), 1)
    sine = inside_ref[1] * cos_s + inside_ref[0] * sin_s
    rope[1] = jnp.where(lanes < HEAD_SIZE // 2, -sine, sine)
    key_token = lax.broadcasted_iota(jnp.int32, (TOK, COLS), 0)
    query_token = lax.rem(lax.broadcasted_iota(jnp.int32, (TOK, COLS), 1), TOK)
    token_gap[...] = key_token - query_token
    inv[...] = jnp.zeros_like(inv)
    pl.semaphore_wait(barrier, len(friends))

    gathers = {
        "wkv": Gather(TREES["wkv"], wkv, wkv_arrive, wkv_handed, wkv_sent, place, False),
        "wq": Gather(TREES["wq"], wq, wq_arrive, wq_handed, wq_sent, place, False),
        "wo": Gather(TREES["wo"], wo, wo_arrive, wo_handed, wo_sent, place, False),
        "k": Gather(TREES["k"], ks, k_arrive, k_handed, k_sent, place, True),
        "v": Gather(TREES["v"], vs, v_arrive, v_handed, v_sent, place, True),
    }

    def remote(src, dst, sent, arrive, device):
        return pltpu.make_async_remote_copy(
            src_ref=src,
            dst_ref=dst,
            send_sem=sent,
            recv_sem=arrive,
            device_id=device,
            device_id_type=MESH_ID,
        )

    part_rows = TOK // HALVES

    def hid_copy(hop, sign, piece, arriving=False):
        source = y_at(-sign * (hop + 1 if arriving else hop))
        block = hid.at[source, pl.ds(piece * part_rows, part_rows)]
        k = (hop * HALVES + piece) * 2 + (sign > 0)
        return remote(block, block, hid_sent.at[k], hid_arrive.at[k], y_near(sign))

    def hid_goes(hop, sign, piece):
        return hop < 3 or (hop == 3 and (piece < HALVES // 2) == (sign > 0))

    def gain_copy(d, source):
        block = gains.at[source]
        return remote(block, block, gain_sent.at[d], gain_arrive.at[d], y_near(d))

    def prepare(source, piece):
        rows = slice(piece * part_rows, (piece + 1) * part_rows)
        h = hid[source, rows].astype(jnp.float32)
        u[source, rows] = (h * gains[source][0:1, :]).astype(jnp.bfloat16)
        squares = h * h
        part = squares[:, 0:128]
        for k in range(1, COLS // 128):
            part = part + squares[:, k * 128 : (k + 1) * 128]
        inv[rows] = inv[rows] + part

    def project(weights, width):
        def step(k, total):
            block = weights[pl.ds(k * (BLOCKS // NY), BLOCKS // NY)].reshape(COLS, width)
            return total + jnp.dot(u[k], block, preferred_element_type=jnp.float32)

        zero = jnp.zeros((TOK, width), jnp.float32)
        return lax.fori_loop(0, NY, step, zero, unroll=True)

    def rotate(head):
        return head * rope[0] + pltpu.roll(head, HEAD_SIZE // 2, 1) * rope[1]

    def make_keys():
        row_sum = jnp.sum(inv[...], axis=1, keepdims=True)
        inv[...] = jnp.broadcast_to(lax.rsqrt(row_sum / MODEL_WIDTH + eps), (TOK, 128))
        pair = project(wkv, 2 * HEAD_SIZE)
        scale = inv[...]
        keys = pair[:, :HEAD_SIZE] * scale + bkv_ref[0:1, :].astype(jnp.float32)
        values = pair[:, HEAD_SIZE:] * scale + bkv_ref[1:2, :].astype(jnp.float32)
        ks[me] = rotate(keys).astype(jnp.bfloat16)
        vs[me] = values.T.astype(jnp.bfloat16)

    def make_query():
        query = project(wq, COLS)
        bias = bq_ref[...].astype(jnp.float32).reshape(1, COLS)
        for g in range(GROUP):
            lanes = slice(g * HEAD_SIZE, (g + 1) * HEAD_SIZE)
            one = rotate(query[:, lanes] * inv[...] + bias[:, lanes])
            qs[g * TOK : (g + 1) * TOK, :] = one.astype(jnp.bfloat16)

    def attend(row):
        first = row == 0
        base = lax.rem(z - row + NZ, NZ) * NX * NC
        count = NX * NC
        keys = ks[pl.ds(base, count)].reshape(count * TOK, HEAD_SIZE)
        scores = lax.dot_general(
            keys, qs[...], (((1,), (1,)), ((), ())), preferred_element_type=jnp.float32
        )
        blocks, shifts, peak = [], [], None
        for k in range(count):
            block = scores[k * TOK : (k + 1) * TOK] * exponent_scale
            ahead = own_span - span_ref[base + k]
            if first:
                block = jnp.where(token_gap[...] <= ahead * TOK, block, -1e30)
                shift = jnp.float32(0.0)
            else:
                shift = jnp.where(ahead > 0, 0.0, 1e30).astype(jnp.float32)
            high = jnp.max(block, axis=0, keepdims=True) - shift
            peak = high if peak is None else jnp.maximum(peak, high)
            blocks.append(block)
            shifts.append(shift)
        if not first:
            old = top[0:1, :]
            peak = jnp.maximum(old, peak)
        weights, sums = [], None
        for block, shift in zip(blocks, shifts):
            w = jnp.exp2(block - (peak + shift))
            part = jnp.sum(w, axis=0, keepdims=True)
            sums = part if sums is None else sums + part
            weights.append(w.astype(jnp.bfloat16))
        values = jnp.concatenate([vs[base + k] for k in range(count)], axis=1)
        summed = jnp.dot(
            values, jnp.concatenate(weights, axis=0), preferred_element_type=jnp.float32
        )
        if not first:
            factor = jnp.exp2(old - peak)
            sums = sums + total[0:1, :] * factor
            summed = summed + acc[...] * factor
        top[0:1, :] = peak
        total[0:1, :] = sums
        acc[...] = summed

    seen_gain = {0}
    for step in planned_steps():
        if step[0] == "hid":
            _, hop, sign, piece = step
            if hop == 0:
                if piece == 0 and sign > 0:
                    starts["hid"].wait()
                hid_copy(0, sign, piece).start()
                if piece == HALVES - 1 and sign < 0:
                    for d in range(1, NY):
                        gain_copy(d, y).start()
                    for k in range(HALVES):
                        prepare(y, k)
            else:
                hid_copy(hop - 1, sign, piece, True).wait_recv()
                if hid_goes(hop, sign, piece):
                    hid_copy(hop, sign, piece).start()
                d = sign * hop % NY
                if d not in seen_gain:
                    seen_gain.add(d)
                    gain_copy(d, y_at(-d)).wait_recv()
                prepare(y_at(-d), piece)
        elif step[0] == "keys":
            gathers["wkv"].wait_handed()
            make_keys()
        elif step[0] == "query":
            gathers["wq"].wait_handed()
            make_query()
        elif step[0] == "attend":
            gathers["k"].wait_handed(step[1] % NZ)
            gathers["v"].wait_handed(step[1] % NZ)
            attend(step[1])
        else:
            g, o = step
            if o == (0, 0) and g in ("wq", "wo"):
                starts[g].wait()
            gathers[g].arrived(o)
    for g in range(GROUP):
        lanes = slice(g * TOK, (g + 1) * TOK)
        one = (acc[:, lanes] / total[0:1, lanes]).T
        attended[:, g * HEAD_SIZE : (g + 1) * HEAD_SIZE] = one.astype(jnp.bfloat16)
    gathers["wo"].wait_handed()

    def partial(target):
        block = wo[pl.ds(target * (BLOCKS // NY), BLOCKS // NY)].reshape(COLS, COLS)
        return lax.dot_general(
            attended[...], block, (((1,), (1,)), ((), ())), preferred_element_type=jnp.float32
        )

    sub = TOK // SUBS
    half = COLS // 2

    def sum_copy(step, sign, piece):
        outs, ins, sent, arrive = (
            (plus_out, plus_in, plus_sent, plus_arrive)
            if sign > 0
            else (minus_out, minus_in, minus_sent, minus_arrive)
        )
        rows = pl.ds(piece * sub, sub)
        lanes = pl.ds(0, COLS)
        if step == 0:
            lanes = pl.ds(0 if sign > 0 else half, half)
        k = step * SUBS + piece
        return remote(
            outs.at[step, rows, lanes],
            ins.at[step, rows, lanes],
            sent.at[k],
            arrive.at[k],
            y_near(sign),
        )

    far = partial(y_at(4)).astype(jnp.bfloat16)
    plus_out[0, :, 0:half] = far[:, :half]
    minus_out[0, :, half:COLS] = far[:, half:]
    for piece in range(SUBS):
        sum_copy(0, 1, piece).start()
        sum_copy(0, -1, piece).start()
    for step in range(1, 4):
        terms = {1: partial(y_at(4 - step)), -1: partial(y_at(step - 4))}
        for piece in range(SUBS):
            rows = slice(piece * sub, (piece + 1) * sub)
            for sign in (1, -1):
                outs, ins = (plus_out, plus_in) if sign > 0 else (minus_out, minus_in)
                sum_copy(step - 1, sign, piece).wait_recv()
                term = terms[sign][rows]
                if step == 1:
                    lanes = slice(0, half) if sign > 0 else slice(half, COLS)
                    other = slice(half, COLS) if sign > 0 else slice(0, half)
                    got = ins[0, rows, lanes].astype(jnp.float32)
                    outs[1, rows, lanes] = (term[:, lanes] + got).astype(jnp.bfloat16)
                    outs[1, rows, other] = term[:, other].astype(jnp.bfloat16)
                else:
                    got = ins[step - 1, rows].astype(jnp.float32)
                    outs[step, rows] = (term + got).astype(jnp.bfloat16)
                sum_copy(step, sign, piece).start()
    own = partial(y)
    for piece in range(SUBS):
        rows = slice(piece * sub, (piece + 1) * sub)
        for sign in (1, -1):
            sum_copy(3, sign, piece).wait_recv()
        mixed = (
            own[rows]
            + plus_in[3, rows].astype(jnp.float32)
            + minus_in[3, rows].astype(jnp.float32)
        )
        mixed_ref[rows, :] = mixed
        both_ref[0, rows, :] = mixed.astype(jnp.bfloat16)
        stream = hid[y, rows].astype(jnp.float32) + mixed
        squares = stream * stream
        part = squares[:, 0:128]
        for k in range(1, COLS // 128):
            part = part + squares[:, k * 128 : (k + 1) * 128]
        inv[rows, :] = part

    column = jnp.sum(inv[...], axis=1, keepdims=True)
    stats[y] = jnp.broadcast_to(column, (TOK, 128)).T[0:8, :]

    def stats_copy(d, source):
        block = stats.at[source]
        return remote(block, block, stats_sent.at[d], stats_arrive.at[d], y_near(d))

    for d in range(1, NY):
        stats_copy(d, y).start()
    for g in gathers.values():
        g.wait_sent()
    for step in range(4):
        for sign in (1, -1):
            for piece in range(HALVES):
                if hid_goes(step, sign, piece):
                    hid_copy(step, sign, piece).wait_send()
            for piece in range(SUBS):
                sum_copy(step, sign, piece).wait_send()
    for d in range(1, NY):
        gain_copy(d, y).wait_send()
    for d in range(1, NY):
        stats_copy(d, y_at(-d)).wait_recv()
    summed = stats[0]
    for k in range(1, NY):
        summed = summed + stats[k]
    rows = jnp.broadcast_to(summed[0:1, :], (128, TOK)).T
    scale = lax.rsqrt(rows / MODEL_WIDTH + eps)
    post = post_ref[...].astype(jnp.float32).reshape(1, COLS)
    for g in range(GROUP):
        lanes = slice(g * 128, (g + 1) * 128)
        stream = hid[y, :, lanes].astype(jnp.float32) + mixed_ref[:, lanes]
        both_ref[1, :, lanes] = (stream * scale * post[:, lanes]).astype(jnp.bfloat16)
    for d in range(1, NY):
        stats_copy(d, y).wait_send()


def per_device(
    hidden_in,
    span_order,
    norm_gain,
    w_query,
    bias_query,
    key_value_weight,
    bias_kv,
    w_out,
    post_gain,
):
    half = HEAD_SIZE // 2
    inverse = rope_base ** (-(np.arange(HEAD_SIZE) % half) / half)
    row_angles = np.arange(TOK)[:, None] * inverse[None, :]
    span_angles = np.arange(BLOCKS)[:, None] * TOK * inverse[None, :]
    inside = np.stack([np.cos(row_angles), np.sin(row_angles)]).astype(np.float32)
    spans = np.stack([np.cos(span_angles), np.sin(span_angles)], axis=1).astype(np.float32)

    bf16, f32 = jnp.bfloat16, jnp.float32
    vmem = pl.BlockSpec(memory_space=pltpu.VMEM)
    anywhere = pl.BlockSpec(memory_space=pl.ANY)
    dma = pltpu.SemaphoreType.DMA
    gathers = []
    for rows in (1, 1, 1, NZ, NZ):
        gathers += [dma((PLANE,)), dma((rows,)), dma((1,))]
    both = pl.pallas_call(
        kernel,
        out_shape=jax.ShapeDtypeStruct((2, TOK, COLS), bf16),
        in_specs=[anywhere] * 11,
        out_specs=vmem,
        scratch_shapes=[
            pltpu.VMEM((TOK, COLS), f32),
            pltpu.VMEM((WROWS, 2, HEAD_SIZE), bf16),
            pltpu.SMEM((BLOCKS,), jnp.int32),
            pltpu.VMEM((COLS,), bf16),
            pltpu.VMEM((COLS,), bf16),
            pltpu.VMEM((2, HEAD_SIZE), bf16),
            pltpu.VMEM((COLS,), bf16),
            pltpu.VMEM((2, TOK, HEAD_SIZE), f32),
            pltpu.VMEM((BLOCKS, 2, HEAD_SIZE), f32),
            pltpu.VMEM((NY, TOK, COLS), bf16),
            pltpu.VMEM((NY, 8, COLS), f32),
            pltpu.VMEM((BLOCKS, WROWS, 2 * HEAD_SIZE), bf16),
            pltpu.VMEM((BLOCKS, WROWS, COLS), bf16),
            pltpu.VMEM((BLOCKS, WROWS, COLS), bf16),
            pltpu.VMEM((BLOCKS, TOK, HEAD_SIZE), bf16),
            pltpu.VMEM((BLOCKS, TOK, HEAD_SIZE), bf16),
            pltpu.VMEM((NY, TOK, COLS), bf16),
            pltpu.VMEM((TOK, 128), f32),
            pltpu.VMEM((2, TOK, 128), f32),
            pltpu.VMEM((TOK, COLS), jnp.int32),
            pltpu.VMEM((COLS, HEAD_SIZE), bf16),
            pltpu.VMEM((8, COLS), f32),
            pltpu.VMEM((8, COLS), f32),
            pltpu.VMEM((HEAD_SIZE, COLS), f32),
            pltpu.VMEM((TOK, COLS), bf16),
            pltpu.VMEM((4, TOK, COLS), bf16),
            pltpu.VMEM((4, TOK, COLS), bf16),
            pltpu.VMEM((4, TOK, COLS), bf16),
            pltpu.VMEM((4, TOK, COLS), bf16),
            pltpu.VMEM((NY, 8, 128), f32),
            dma((11,)),
            dma((8 * HALVES,)),
            dma((8 * HALVES,)),
            dma((NY,)),
            dma((NY,)),
            *gathers,
            dma((4 * SUBS,)),
            dma((4 * SUBS,)),
            dma((4 * SUBS,)),
            dma((4 * SUBS,)),
            dma((NY,)),
            dma((NY,)),
        ],
        compiler_params=pltpu.CompilerParams(
            collective_id=0, has_side_effects=True, vmem_limit_bytes=56 << 20
        ),
    )(
        hidden_in,
        w_query,
        key_value_weight,
        w_out.T,
        span_order,
        norm_gain,
        bias_query,
        bias_kv,
        post_gain,
        jnp.asarray(inside),
        jnp.asarray(spans),
    )
    return both[0], both[1]


def solution(mesh):
    torus = Mesh(mesh.devices.reshape(NZ, NX, NC, NY), ("z", "x", "c", "y"))
    in_specs = (
        P(SEQ, "y"),
        P(),
        P("y"),
        P(SEQ, "y"),
        P("y"),
        P(SEQ, None, "y"),
        P(None, "y"),
        P("y", SEQ),
        P("y"),
    )
    out_specs = (P(SEQ, "y"), P(SEQ, "y"))
    return jax.shard_map(
        per_device, mesh=torus, in_specs=in_specs, out_specs=out_specs, check_vma=False
    )
```
